32 devices in a mesh: grp: 1, sp: 4 (over z), blk: 4 (over y, x), rep: 2 (over core).
Axes of the slice: x: 2, y: 2, z: 4, core: 2. Of those that a mesh axis runs over, the one named last changes fastest.
Arguments:
- hidden: bfloat16 [4, 512, 4096], P(('grp', 'blk'), 'sp'), may hold values from -64 to 64
- queries: bfloat16 [4, 512, 4096], P(('grp', 'blk'), 'sp', 'rep'), may hold values from -600 to 600
- norm_gain: float32 [4096], replicated, may hold values from 0.1 to 1.9
- key_matrix: bfloat16 [4096, 1024], P('sp', 'rep'), may hold values from -0.09375 to 0.09375
- value_matrix: bfloat16 [4096, 1024], P('sp', 'rep'), may hold values from -0.09375 to 0.09375
- key_shift_bias: bfloat16 [1024], P('rep'), may hold values from -3 to 3
- value_shift_bias: bfloat16 [1024], P('rep'), may hold values from -3 to 3
- doc_lengths: int32 [8], P('grp'), may hold values from 1 to 1025, 2048 in all
Outputs:
- attended: bfloat16 [4, 512, 4096], P(('grp', 'blk'), 'sp', 'rep')
The draws below stay inside these ranges and needn't reach their ends.
Inputs may be any that keep to these rules, and one draw needn't show every extreme that they name: `doc_lengths`: the lengths of the 8 documents packed in order into the sequence; they sum to 2048, and the longest is exactly 1025 tokens.
All inputs are finite; a program needn't handle non-finite values.
Results may differ from the reference program's by a relative error of at most 0.012.
The reference program's roundings to bfloat16 on the way count: a program that leaves them out, or rounds other values in their place, can miss the bound.
Values may be sent and summed in bfloat16 or wider, within the bound.
A program may use at most 64 MiB of HBM per device.

```python
import math
import jax
import jax.numpy as jnp
import numpy as np
from jax import lax

MODEL_WIDTH = 4096
QUERY_HEADS = 32
KEY_VALUE_HEADS = 8
HEAD_DIMENSION = 128
DOCS = 8
CH = 512
SEQUENCE_TOKENS = 2048
DOC_MOST = 1025


def draw_queries(key, part):
    first_key = jax.random.fold_in(jax.random.fold_in(key, 11), 0)
    full_shape = (SEQUENCE_TOKENS // CH, CH, QUERY_HEADS * HEAD_DIMENSION)
    drawn = jnp.clip(jax.random.normal(first_key, full_shape, jnp.float32), -4.0, 4.0)
    return drawn.astype(jnp.bfloat16)


def draw_hidden(key, part):
    first_key = jax.random.fold_in(jax.random.fold_in(key, 23), 0)
    full_shape = (SEQUENCE_TOKENS // CH, CH, MODEL_WIDTH)
    drawn = jnp.clip(jax.random.normal(first_key, full_shape, jnp.float32), -5.0, 5.0)
    return drawn.astype(jnp.bfloat16)


def level_of(key, dims, cuts, smallest, high):
    def one(axis_at, blocks):
        heights = jax.random.uniform(jax.random.fold_in(jax.random.fold_in(key, 6), axis_at), (blocks,), jnp.float32, smallest / len(cuts), high / len(cuts))
        return jnp.repeat(jnp.exp(heights), dims[axis_at] // blocks).reshape((-1,) + (1,) * (len(dims) - axis_at - 1))

    level = one(*cuts[0])
    for cut in cuts[1:]:
        level = level * one(*cut)
    return level


def profile(amount, total, bound, slope):
    loads = [(1 << 20) // math.isqrt(standing ** slope) + 1 for standing in range(2, amount + 1)]
    spare, given = total - bound - (amount - 1), [1] * (amount - 1)
    while spare > 0:
        candidates = [i for i in range(amount - 1) if given[i] < bound]
        pool, remaining = sum([loads[i] for i in candidates]), spare
        for i in candidates:
            extra = min(bound - given[i], max(1, remaining * loads[i] // pool), spare)
            given[i] = given[i] + extra
            spare = spare - extra
    return np.array([bound] + given)


def ragged(stream_key, amount, total, most, skew):
    if amount == 2:
        one = jax.random.randint(stream_key, (), max(1, total - most), min(most, total - 1) + 1)
        return jnp.stack([one, total - one])
    tallies = jnp.asarray(profile(amount, total, most, skew), jnp.int32)
    couples = (amount - 1) // 2
    giver, receiver = tallies[1:1 + 2 * couples:2], tallies[2:2 + 2 * couples:2]
    room = jnp.minimum(giver - 1, most - receiver)
    shifted = jax.random.randint(jax.random.fold_in(stream_key, 1), (couples,), 0, 1 << 20) % (room + 1)
    tallies = tallies.at[1:1 + 2 * couples:2].set(giver - shifted).at[2:2 + 2 * couples:2].set(receiver + shifted)
    return tallies[jax.random.permutation(jax.random.fold_in(stream_key, 2), amount)]


def centred(own_key, extent, width, most, shards=(), dtype=jnp.bfloat16):
    loudness = level_of(own_key, extent, shards, -0.22, 0.18) if shards else 1.0
    entries = jax.random.normal(own_key, extent, jnp.float32) * width * loudness
    return jnp.minimum(jnp.maximum(entries, -most), most).astype(dtype)


def setup_inputs(seed: int = 0, part: int = 0) -> dict:
    key_list = jax.random.split(jax.random.key(seed), 9)
    own_keys = jax.random.split(jax.random.fold_in(key_list[8], part), 9)
    return {
        "hidden": draw_hidden(jax.random.fold_in(jax.random.fold_in(key_list[8], part), 71), part),
        "queries": draw_queries(jax.random.fold_in(jax.random.fold_in(key_list[8], part), 71), part),
        "norm_gain": jnp.clip(1.0 + 0.18 * jax.random.normal(key_list[2], (MODEL_WIDTH,), jnp.float32), 0.1, 1.9),
        "key_matrix": centred(key_list[3], (MODEL_WIDTH, KEY_VALUE_HEADS * HEAD_DIMENSION), MODEL_WIDTH ** -0.5, 0.09375, ((0, 4), (1, 2))),
        "value_matrix": centred(key_list[4], (MODEL_WIDTH, KEY_VALUE_HEADS * HEAD_DIMENSION), MODEL_WIDTH ** -0.5, 0.09375, ((0, 4), (1, 2))),
        "key_shift_bias": centred(key_list[5], (KEY_VALUE_HEADS * HEAD_DIMENSION,), 0.5, 3.0, ((0, 2),)),
        "value_shift_bias": centred(key_list[6], (KEY_VALUE_HEADS * HEAD_DIMENSION,), 0.5, 3.0, ((0, 2),)),
        "doc_lengths": ragged(own_keys[7], DOCS, SEQUENCE_TOKENS, DOC_MOST, 2).astype(jnp.int32),
    }


EPS_VALUE = 1e-06
THETA_BASE = 1000000.0

def apply_rotation(projected, token_places):
    half_size = projected.shape[-1] // 2
    freq_index = jnp.arange(half_size).astype(jnp.float32)
    inverse = jnp.exp(freq_index * (-2.0 * math.log(THETA_BASE) / projected.shape[-1]))
    angles = token_places[:, None] * inverse[None, :]
    cosine = jnp.cos(angles)[:, None, :]
    sine = jnp.sin(angles)[:, None, :]
    first_half = projected[..., :half_size]
    second_half = projected[..., half_size:]
    return jnp.concatenate([first_half * cosine - second_half * sine, second_half * cosine + first_half * sine], axis=-1)

def doc_index(token_places, doc_lengths):
    ending = jnp.cumsum(doc_lengths).astype(jnp.int32)
    return lax.optimization_barrier(jnp.sum((token_places[:, None] >= ending[None, :]).astype(jnp.int32), axis=1))

def reference(hidden, queries, norm_gain, key_matrix, value_matrix, key_shift_bias, value_shift_bias, doc_lengths):
    rows_all = hidden.reshape(SEQUENCE_TOKENS, MODEL_WIDTH).astype(jnp.float32)
    row_scale = lax.rsqrt(lax.optimization_barrier(jnp.mean(rows_all * rows_all, axis=1, keepdims=True)) + EPS_VALUE)
    normed = (rows_all * row_scale * norm_gain.astype(jnp.float32)).astype(jnp.bfloat16)
    token_places = jnp.arange(SEQUENCE_TOKENS).astype(jnp.int32)
    key_projector = jnp.dot(normed, key_matrix, preferred_element_type=jnp.float32) + key_shift_bias.astype(jnp.float32)
    value_projector = jnp.dot(normed, value_matrix, preferred_element_type=jnp.float32) + value_shift_bias.astype(jnp.float32)
    key_vectors = apply_rotation(key_projector.reshape(SEQUENCE_TOKENS, KEY_VALUE_HEADS, HEAD_DIMENSION), token_places.astype(jnp.float32)).astype(jnp.bfloat16)
    value_vectors = value_projector.reshape(SEQUENCE_TOKENS, KEY_VALUE_HEADS, HEAD_DIMENSION).astype(jnp.bfloat16)
    segment = doc_index(token_places, doc_lengths)
    visible = (token_places[None, :] <= token_places[:, None]) & (segment[None, :] == segment[:, None])
    query_heads = queries.reshape(SEQUENCE_TOKENS, QUERY_HEADS, HEAD_DIMENSION).transpose(1, 0, 2)
    heads_of_keys = jnp.repeat(key_vectors.transpose(1, 0, 2), QUERY_HEADS // KEY_VALUE_HEADS, axis=0)
    heads_of_values = jnp.repeat(value_vectors.transpose(1, 0, 2), QUERY_HEADS // KEY_VALUE_HEADS, axis=0)
    scale_factor = 1.0 / math.sqrt(HEAD_DIMENSION)

    def one_head(triple):
        query_rows, key_rows, value_rows = triple
        scores = jnp.dot(query_rows, key_rows.T, preferred_element_type=jnp.float32) * scale_factor
        scores = jnp.where(visible, scores, -1e+30)
        largest = lax.optimization_barrier(jnp.max(scores, axis=1, keepdims=True))
        weights = jnp.where(visible, jnp.exp(scores - largest), 0.0).astype(jnp.bfloat16)
        total = lax.optimization_barrier(jnp.sum(weights.astype(jnp.float32), axis=1, keepdims=True))
        summed = jnp.dot(weights, value_rows, preferred_element_type=jnp.float32)
        return (summed / total).astype(jnp.bfloat16)
    result = lax.map(one_head, (query_heads, heads_of_keys, heads_of_values))
    return result.transpose(1, 0, 2).reshape(SEQUENCE_TOKENS // CH, CH, QUERY_HEADS * HEAD_DIMENSION)
```

```python
import functools
import math

import jax
import jax.numpy as jnp
from jax import lax
from jax.experimental import pallas as pl
from jax.experimental.pallas import tpu as pltpu
from jax.sharding import PartitionSpec as P

HEAD = 128
EPS_VALUE = 1e-06
THETA_BASE = 1000000.0
NEG_FILL = -1e30
MESH = pl.DeviceIdType.MESH
F32, BF16 = jnp.float32, jnp.bfloat16


def kernel(
    sizes,
    hidden_ref,
    queries_ref,
    gain_ref,
    kw_ref,
    vw_ref,
    kb_ref,
    vb_ref,
    docs_ref,
    out_ref,
    hid,
    wts,
    normed,
    feats,
    part_own,
    part_out,
    pair_in,
    pair_out,
    part_in,
    kv,
    qbuf,
    obuf,
    cos_buf,
    sin_buf,
    mask_buf,
    load_sem,
    feat_send,
    feat_recv,
    fwd_send,
    fwd_recv,
    q_send,
    q_recv,
    pair_send,
    pair_recv,
    part_send,
    part_recv,
    kv_send,
    kv_recv,
    o_send,
    o_recv,
):
    sp, blks, reps, rows = sizes
    me = lax.axis_index("sp")
    blk = lax.axis_index("blk")
    rep = lax.axis_index("rep")
    half = rows // reps
    span = sp * rows
    fs = kw_ref.shape[0]
    kv_heads = kw_ref.shape[1] // HEAD
    fold = sp // kv_heads
    my_head = me // fold
    q_cols = queries_ref.shape[2] // sp
    heads = q_cols // HEAD
    window = 2 * span + rows
    docs = docs_ref.shape[0]

    pairs = sp // 2
    my_pair = me // 2
    parity = lax.rem(me, 2)
    slots = pair_in.shape[0]

    def place(k):
        pair = lax.rem(my_pair + k // 2, pairs)
        return 2 * pair + lax.rem(parity + lax.rem(k, 2), 2)

    peer = place
    partner = place(1)

    def slot_head(slot, side):
        return slot if fold > 1 else 2 * slot + side

    barrier = pltpu.get_barrier_semaphore()
    for k in range(1, sp):
        pl.semaphore_signal(barrier, inc=1, device_id={"sp": peer(k)}, device_id_type=MESH)
    for k in range(1, reps):
        pl.semaphore_signal(
            barrier, inc=1, device_id={"rep": lax.rem(rep + k, reps)}, device_id_type=MESH
        )
    for dist in (1, 2):
        pl.semaphore_signal(
            barrier, inc=1, device_id={"blk": lax.rem(blk + dist, blks)}, device_id_type=MESH
        )
        pl.semaphore_signal(
            barrier, inc=1, device_id={"blk": lax.rem(blk + blks - dist, blks)}, device_id_type=MESH
        )

    load_hid = pltpu.make_async_copy(
        hidden_ref.at[0, pl.ds(pl.multiple_of(rep * half, half), half)], hid, load_sem.at[0]
    )
    load_k = pltpu.make_async_copy(kw_ref, wts.at[:, : kv_heads * HEAD], load_sem.at[1])
    load_v = pltpu.make_async_copy(vw_ref, wts.at[:, kv_heads * HEAD :], load_sem.at[2])
    load_q = pltpu.make_async_copy(
        queries_ref.at[0, :, pl.ds(pl.multiple_of(me * q_cols, q_cols), q_cols)],
        qbuf.at[me],
        load_sem.at[3],
    )
    load_hid.start()
    load_k.start()
    load_v.start()
    load_q.start()

    load_hid.wait()
    values = hid[...].astype(F32)
    scale = lax.rsqrt(jnp.mean(values * values, axis=1, keepdims=True) + EPS_VALUE)
    for d in range(sp):
        cols = slice(d * fs, (d + 1) * fs)
        normed[d] = (hid[:, cols].astype(F32) * scale * gain_ref[:, cols]).astype(BF16)

    pl.semaphore_wait(barrier, sp - 1 + reps - 1 + 4)

    def feat_copy(k):
        d = peer(k)
        return pltpu.make_async_remote_copy(
            src_ref=normed.at[d],
            dst_ref=feats.at[me, rep],
            send_sem=feat_send.at[d],
            recv_sem=feat_recv.at[me],
            device_id={"sp": d},
            device_id_type=MESH,
        )

    def feat_arrival(s):
        return pltpu.make_async_remote_copy(
            src_ref=normed.at[0],
            dst_ref=feats.at[s, rep],
            send_sem=feat_send.at[0],
            recv_sem=feat_recv.at[s],
            device_id={"sp": s},
            device_id_type=MESH,
        )

    other = lax.rem(rep + 1, reps)

    def fwd_copy(s, source):
        return pltpu.make_async_remote_copy(
            src_ref=source,
            dst_ref=feats.at[s, rep],
            send_sem=fwd_send.at[s],
            recv_sem=fwd_recv.at[s],
            device_id={"rep": other},
            device_id_type=MESH,
        )

    def fwd_arrival(s):
        return pltpu.make_async_remote_copy(
            src_ref=normed.at[0],
            dst_ref=feats.at[s, other],
            send_sem=fwd_send.at[s],
            recv_sem=fwd_recv.at[s],
            device_id={"rep": other},
            device_id_type=MESH,
        )

    order = list(range(1, sp))
    for k in order:
        feat_copy(k).start()
    fwd_copy(me, normed.at[me]).start()
    feats[me, rep] = normed[me]

    token_base = blk * span
    lanes = lax.broadcasted_iota(jnp.int32, (1, HEAD), 1)
    index = lax.rem(lanes, HEAD // 2).astype(F32)
    inverse = jnp.exp(index * (-2.0 * math.log(THETA_BASE) / HEAD))
    sign = jnp.where(lanes < HEAD // 2, -1.0, 1.0)

    def angle_step(j, carry):
        at = pl.ds(pl.multiple_of(j * rows, rows), rows)
        places = token_base + j * rows + lax.broadcasted_iota(jnp.int32, (rows, HEAD), 0)
        angles = places.astype(F32) * inverse
        cos_buf[at, :] = jnp.cos(angles)
        sin_buf[at, :] = jnp.sin(angles) * sign
        return carry

    lax.fori_loop(0, sp, angle_step, 0)
    load_k.wait()
    load_v.wait()

    def rows_of(j):
        return pl.ds(pl.multiple_of(j * rows, rows), rows)

    def pair_copy(slot, j):
        return pltpu.make_async_remote_copy(
            src_ref=part_out.at[slot_head(slot, 1 - parity), rows_of(j)],
            dst_ref=pair_in.at[slot, rows_of(j)],
            send_sem=pair_send.at[slot],
            recv_sem=pair_recv.at[slot, j],
            device_id={"sp": partner},
            device_id_type=MESH,
        )

    def part_copy(d, j):
        slot = d // fold if fold > 1 else d // 2
        return pltpu.make_async_remote_copy(
            src_ref=pair_out.at[slot, rows_of(j)],
            dst_ref=part_in.at[my_pair, rows_of(j)],
            send_sem=part_send.at[d // 2],
            recv_sem=part_recv.at[my_pair, j],
            device_id={"sp": d},
            device_id_type=MESH,
        )

    def far(k):
        return 2 * lax.rem(my_pair + k, pairs) + parity

    def project(j):
        at = rows_of(j)
        block = feats[j].reshape(rows, fs)
        partial = jnp.dot(block, wts[...], preferred_element_type=F32)
        for h in range(kv_heads):
            key_part = partial[:, h * HEAD : (h + 1) * HEAD]
            value_part = partial[:, (kv_heads + h) * HEAD : (kv_heads + h + 1) * HEAD]
            part_own[h, at, :HEAD] = key_part
            part_own[h, at, HEAD:] = value_part
            part_out[h, at, :HEAD] = key_part.astype(BF16)
            part_out[h, at, HEAD:] = value_part.astype(BF16)
        for slot in range(slots):
            pair_copy(slot, j).start()

    def cross(j):
        at = rows_of(j)
        for slot in range(slots):
            pair_copy(slot, j).wait_recv()
            both = part_own[slot_head(slot, parity), at, :] + pair_in[slot, at, :].astype(F32)
            part_own[slot_head(slot, parity), at, :] = both
            pair_out[slot, at, :] = both.astype(BF16)
        for k in range(1, pairs):
            part_copy(far(k), j).start()

    fwd_arrival(me).wait_recv()
    project(me)

    def arrive(k, carry):
        s = place(k)
        feat_arrival(s).wait_recv()
        fwd_copy(s, feats.at[s, rep]).start()
        fwd_arrival(s).wait_recv()
        project(s)
        cross(place(k - 1))
        return carry

    lax.fori_loop(1, sp, arrive, 0)
    cross(place(sp - 1))

    def q_copy(d):
        return pltpu.make_async_remote_copy(
            src_ref=queries_ref.at[0, :, pl.ds(pl.multiple_of(d * q_cols, q_cols), q_cols)],
            dst_ref=qbuf.at[me],
            send_sem=q_send.at[d],
            recv_sem=q_recv.at[me],
            device_id={"sp": d},
            device_id_type=MESH,
        )

    def q_arrival(s):
        return pltpu.make_async_remote_copy(
            src_ref=qbuf.at[s],
            dst_ref=qbuf.at[s],
            send_sem=q_send.at[s],
            recv_sem=q_recv.at[s],
            device_id={"sp": s},
            device_id_type=MESH,
        )

    for k in reversed(order):
        q_copy(peer(k)).start()

    for piece in (0, 1):

        @pl.when(blk < 2 - piece)
        def _():
            kv[pl.ds(piece * span, span), :] = jnp.zeros((span, 2 * HEAD), BF16)


    def own_shift(ref):
        row = ref[...].astype(F32).reshape(1, kv_heads * HEAD)
        mine = row[:, :HEAD]
        for h in range(1, kv_heads):
            mine = jnp.where(my_head == h, row[:, h * HEAD : (h + 1) * HEAD], mine)
        return mine

    key_shift = own_shift(kb_ref)
    value_shift = own_shift(vb_ref)

    relay = blks == 4

    def kv_copy(piece, dist, j):
        return pltpu.make_async_remote_copy(
            src_ref=kv.at[pl.ds(pl.multiple_of(piece * span + j * rows, rows), rows)],
            dst_ref=kv.at[pl.ds(pl.multiple_of((2 - dist) * span + j * rows, rows), rows)],
            send_sem=kv_send.at[dist - 1],
            recv_sem=kv_recv.at[dist - 1, j],
            device_id={"blk": lax.rem(blk + dist, blks)},
            device_id_type=MESH,
        )

    def kv_pass(j):
        kv_copy(2, 2, j).wait_recv()
        pltpu.make_async_remote_copy(
            src_ref=kv.at[pl.ds(pl.multiple_of(j * rows, rows), rows)],
            dst_ref=kv.at[pl.ds(pl.multiple_of(span + j * rows, rows), rows)],
            send_sem=kv_send.at[0],
            recv_sem=kv_recv.at[0, j],
            device_id={"blk": lax.rem(blk + blks - 1, blks)},
            device_id_type=MESH,
        ).start()

    near = blk + 1 < blks
    if relay:
        near = near & (blk != 1)
    sends = {1: near, 2: blk + 2 < blks}

    def finish(i, carry):
        j = place(i)
        at = rows_of(j)
        total = part_own[my_head, at, :]
        for k in range(1, pairs):
            s = lax.rem(my_pair + k, pairs)
            pltpu.make_async_remote_copy(
                src_ref=part_in.at[s, at],
                dst_ref=part_in.at[s, at],
                send_sem=part_send.at[s],
                recv_sem=part_recv.at[s, j],
                device_id={"sp": far(k)},
                device_id_type=MESH,
            ).wait_recv()
            total = total + part_in[s, at, :].astype(F32)
        keys = total[:, :HEAD] + key_shift
        turned = keys * cos_buf[at, :] + pltpu.roll(keys, HEAD // 2, 1) * sin_buf[at, :]
        put = pl.ds(pl.multiple_of(2 * span + j * rows, rows), rows)
        kv[put, :HEAD] = turned.astype(BF16)
        kv[put, HEAD:] = (total[:, HEAD:] + value_shift).astype(BF16)
        for dist in (2, 1):

            @pl.when(sends[dist])
            def _():
                kv_copy(2, dist, j).start()

        if relay:

            @pl.when((blk == 3) & (i >= 1))
            def _():
                kv_pass(place(i - 1))

        return carry

    lax.fori_loop(0, sp, finish, 0)
    if relay:

        @pl.when(blk == 3)
        def _():
            kv_pass(place(sp - 1))


    ends = []
    running = jnp.int32(0)
    for d in range(docs):
        running = running + docs_ref[d]
        ends.append(running)

    load_q.wait()
    for dist in (1, 2):

        arrives = blk >= dist
        if relay and dist == 2:
            arrives = arrives & (blk != 3)

        @pl.when(arrives)
        def _():
            for j in range(sp):
                kv_copy(2, dist, j).wait_recv()

    exponent = math.log2(math.e) / math.sqrt(HEAD)

    def attend(t):
        query_at = token_base + t * rows + lax.broadcasted_iota(jnp.int32, (rows, HEAD), 0)
        first = jnp.zeros((rows, HEAD), jnp.int32)
        for end in ends:
            first = jnp.where(query_at >= end, end, first)
        key_base = token_base - 2 * span + t * rows
        for c in range(window // HEAD):
            key_at = key_base + c * HEAD + lax.broadcasted_iota(jnp.int32, (rows, HEAD), 1)
            seen = (key_at >= first) & (key_at <= query_at)
            mask_buf[:, c * HEAD : (c + 1) * HEAD] = jnp.where(seen, 0.0, NEG_FILL)
        at = pl.ds(pl.multiple_of(t * rows, rows), window)
        for h in range(heads):
            cols = slice(h * HEAD, (h + 1) * HEAD)
            scores = lax.dot_general(
                qbuf[t, :, cols], kv[at, :HEAD], (((1,), (1,)), ((), ())), preferred_element_type=F32
            )
            scores = scores + mask_buf[...]
            largest = jnp.max(scores, axis=1, keepdims=True)
            weights = jnp.exp2((scores - largest) * exponent).astype(BF16)
            total = jnp.sum(weights.astype(F32), axis=1, keepdims=True)
            summed = jnp.dot(weights, kv[at, HEAD:], preferred_element_type=F32)
            obuf[t, :, cols] = (summed / total).astype(BF16)

    my_cols = pl.ds(pl.multiple_of(me * q_cols, q_cols), q_cols)

    def o_copy(d):
        return pltpu.make_async_remote_copy(
            src_ref=obuf.at[d],
            dst_ref=out_ref.at[0, :, my_cols],
            send_sem=o_send.at[d],
            recv_sem=o_recv.at[me],
            device_id={"sp": d},
            device_id_type=MESH,
        )

    def o_arrival(s):
        return pltpu.make_async_remote_copy(
            src_ref=obuf.at[s],
            dst_ref=out_ref.at[0, :, pl.ds(pl.multiple_of(s * q_cols, q_cols), q_cols)],
            send_sem=o_send.at[s],
            recv_sem=o_recv.at[s],
            device_id={"sp": s},
            device_id_type=MESH,
        )

    def each(k, carry):
        t = place(sp - k)
        q_arrival(t).wait_recv()
        attend(t)
        o_copy(t).start()
        return carry

    lax.fori_loop(1, sp, each, 0)
    attend(me)
    out_ref[0, :, my_cols] = obuf[me]

    for k in order:
        d = peer(k)
        o_arrival(d).wait_recv()
        o_copy(d).wait_send()
        feat_copy(k).wait_send()
        q_copy(d).wait_send()
        fwd_copy(d, feats.at[d, rep]).wait_send()
    fwd_copy(me, normed.at[me]).wait_send()

    def sent(sem, source):
        pltpu.make_async_remote_copy(
            src_ref=source,
            dst_ref=source,
            send_sem=sem,
            recv_sem=part_recv.at[0, 0],
            device_id={"sp": partner},
            device_id_type=MESH,
        ).wait_send()

    for slot in range(slots):
        sent(pair_send.at[slot], pair_in.at[slot])
    for k in range(1, pairs):
        sent(part_send.at[far(k) // 2], part_in.at[0])
    for dist in (1, 2):

        shipped = sends[dist]
        if relay and dist == 1:
            shipped = shipped | (blk == 3)

        @pl.when(shipped)
        def _():
            sent(kv_send.at[dist - 1], kv.at[pl.ds(0, span)])


def heads_kernel(
    sizes,
    hidden_ref,
    queries_ref,
    gain_ref,
    kw_ref,
    vw_ref,
    kb_ref,
    vb_ref,
    docs_ref,
    out_ref,
    hid,
    wts,
    normed,
    feats,
    own,
    up_in,
    up_out,
    down_in,
    down_out,
    self_out,
    self_in,
    up_last,
    down_last,
    kv,
    qbuf,
    obuf,
    total,
    cos_buf,
    sin_buf,
    mask_buf,
    load_sem,
    feat_send,
    feat_recv,
    fwd_send,
    fwd_recv,
    q_send,
    q_recv,
    self_send,
    self_recv,
    up_send,
    up_recv,
    up_last_send,
    up_last_recv,
    down_send,
    down_recv,
    down_last_send,
    down_last_recv,
    rise_send,
    rise_recv,
    fall_send,
    fall_recv,
    o_send,
    o_recv,
):
    sp, blks, reps, rows, chunks = sizes
    me = lax.axis_index("sp")
    blk = lax.axis_index("blk")
    rep = lax.axis_index("rep")
    span = sp * rows
    cut = rows // chunks
    part = cut // reps
    fs = kw_ref.shape[0]
    q_cols = queries_ref.shape[2] // blks
    heads = q_cols // HEAD
    docs = docs_ref.shape[0]
    window = 2 * span + rows
    last = sp - 1
    pair = 2 * HEAD

    def group(k):
        return lax.rem(blk + k, blks)

    barrier = pltpu.get_barrier_semaphore()
    for k in range(1, sp):
        pl.semaphore_signal(
            barrier, inc=1, device_id={"sp": lax.rem(me + k, sp)}, device_id_type=MESH
        )
    for k in range(1, reps):
        pl.semaphore_signal(
            barrier, inc=1, device_id={"rep": lax.rem(rep + k, reps)}, device_id_type=MESH
        )
    for k in range(1, blks):
        pl.semaphore_signal(barrier, inc=1, device_id={"blk": group(k)}, device_id_type=MESH)

        @pl.when(me > 0)
        def _():
            pl.semaphore_signal(
                barrier, inc=1, device_id={"sp": me - 1, "blk": group(k)}, device_id_type=MESH
            )

        @pl.when(me < last)
        def _():
            pl.semaphore_signal(
                barrier, inc=1, device_id={"sp": me + 1, "blk": group(k)}, device_id_type=MESH
            )

    def load_hid(q):
        return pltpu.make_async_copy(
            hidden_ref.at[0, pl.ds(pl.multiple_of(q * cut + rep * part, part), part)],
            hid.at[q],
            load_sem.at[q],
        )

    def load_w(g, side):
        source = vw_ref if side else kw_ref
        return pltpu.make_async_copy(
            source.at[:, g * HEAD : (g + 1) * HEAD],
            wts.at[:, (2 * g + side) * HEAD : (2 * g + side + 1) * HEAD],
            load_sem.at[chunks + 2 * g + side],
        )

    own_cols = pl.ds(pl.multiple_of(blk * q_cols, q_cols), q_cols)
    load_q = pltpu.make_async_copy(
        queries_ref.at[0, :, own_cols], qbuf.at[blk], load_sem.at[chunks + 2 * blks]
    )
    for q in range(chunks):
        load_hid(q).start()
    for g in range(blks):
        load_w(g, 0).start()
        load_w(g, 1).start()
    load_q.start()

    def feat_copy(q, d):
        return pltpu.make_async_remote_copy(
            src_ref=normed.at[q, d],
            dst_ref=feats.at[q, me, rep],
            send_sem=feat_send,
            recv_sem=feat_recv.at[q, me],
            device_id={"sp": d},
            device_id_type=MESH,
        )

    def feat_arrival(q, s):
        return pltpu.make_async_remote_copy(
            src_ref=normed.at[q, 0],
            dst_ref=feats.at[q, s, rep],
            send_sem=feat_send,
            recv_sem=feat_recv.at[q, s],
            device_id={"sp": s},
            device_id_type=MESH,
        )

    other = lax.rem(rep + 1, reps)

    def fwd_copy(q, s, source):
        return pltpu.make_async_remote_copy(
            src_ref=source,
            dst_ref=feats.at[q, s, rep],
            send_sem=fwd_send,
            recv_sem=fwd_recv.at[q],
            device_id={"rep": other},
            device_id_type=MESH,
        )

    def q_copy(g):
        return pltpu.make_async_remote_copy(
            src_ref=queries_ref.at[0, :, pl.ds(pl.multiple_of(g * q_cols, q_cols), q_cols)],
            dst_ref=qbuf.at[blk],
            send_sem=q_send,
            recv_sem=q_recv,
            device_id={"blk": g},
            device_id_type=MESH,
        )

    def norm(q):
        load_hid(q).wait()
        values = hid[q].astype(F32)
        scale = lax.rsqrt(jnp.mean(values * values, axis=1, keepdims=True) + EPS_VALUE)
        for d in range(sp):
            cols = slice(d * fs, (d + 1) * fs)
            normed[q, d] = (hid[q, :, cols].astype(F32) * scale * gain_ref[:, cols]).astype(BF16)

    for q in range(chunks):
        norm(q)
    peers = sp - 1 + reps - 1 + blks - 1

    @pl.when((me == 0) | (me == last))
    def _():
        pl.semaphore_wait(barrier, peers + blks - 1)

    @pl.when((me > 0) & (me < last))
    def _():
        pl.semaphore_wait(barrier, peers + 2 * (blks - 1))

    for q in range(chunks):
        for step in range(1, sp):
            far = jnp.where(rep == 0, step, sp - step)

            @pl.when(me + far < sp)
            def _():
                feat_copy(q, me + far).start()

            @pl.when(me >= far)
            def _():
                feat_copy(q, me - far).start()

        fwd_copy(q, me, normed.at[q, me]).start()
        feats[q, me, rep] = normed[q, me]
    for k in range(1, blks):
        q_copy(group(k)).start()

    lanes = lax.broadcasted_iota(jnp.int32, (1, HEAD), 1)
    index = lax.rem(lanes, HEAD // 2).astype(F32)
    inverse = jnp.exp(index * (-2.0 * math.log(THETA_BASE) / HEAD))
    sign = jnp.where(lanes < HEAD // 2, -1.0, 1.0)

    def angle_step(c, carry):
        places = c * span + me * rows + lax.broadcasted_iota(jnp.int32, (rows, HEAD), 0)
        angles = places.astype(F32) * inverse
        cos_buf[c] = jnp.cos(angles)
        sin_buf[c] = jnp.sin(angles) * sign
        return carry

    lax.fori_loop(0, blks, angle_step, 0)
    kv[: 2 * span, :pair] = jnp.zeros((2 * span, pair), BF16)
    kv[:, pair:] = jnp.ones((kv.shape[0], HEAD), BF16)

    def own_shift(ref):
        row = ref[...].astype(F32).reshape(1, blks * HEAD)
        mine = row[:, :HEAD]
        for g in range(1, blks):
            mine = jnp.where(blk == g, row[:, g * HEAD : (g + 1) * HEAD], mine)
        return mine

    key_shift = own_shift(kb_ref)
    value_shift = own_shift(vb_ref)

    def landed(sem, ref):
        pltpu.make_async_remote_copy(
            src_ref=ref,
            dst_ref=ref,
            send_sem=sem,
            recv_sem=sem,
            device_id={"rep": other},
            device_id_type=MESH,
        ).wait_recv()

    def left(sem, ref):
        pltpu.make_async_remote_copy(
            src_ref=ref,
            dst_ref=ref,
            send_sem=sem,
            recv_sem=sem,
            device_id={"rep": other},
            device_id_type=MESH,
        ).wait_send()

    def self_copy(q, g):
        return pltpu.make_async_remote_copy(
            src_ref=self_out.at[q, g],
            dst_ref=self_in.at[q, blk],
            send_sem=self_send,
            recv_sem=self_recv.at[q],
            device_id={"blk": g},
            device_id_type=MESH,
        )

    def project(q):
        for far in range(1, sp):

            @pl.when(me >= far)
            def _():
                feat_arrival(q, me - far).wait_recv()
                fwd_copy(q, me - far, feats.at[q, me - far, rep]).start()

            @pl.when(me + far < sp)
            def _():
                feat_arrival(q, me + far).wait_recv()
                fwd_copy(q, me + far, feats.at[q, me + far, rep]).start()

        landed(fwd_recv.at[q], normed.at[q])
        partial = jnp.dot(
            feats[q].reshape(sp * cut, fs), wts[...], preferred_element_type=F32
        )
        for j in range(sp):
            for g in range(blks):
                own[q, j, g] = partial[j * cut : (j + 1) * cut, g * pair : (g + 1) * pair]

    def keep(q):
        for k in range(1, blks):
            g = group(k)
            self_out[q, g] = own[q, me, g].astype(BF16)
            self_copy(q, g).start()
        self_in[q, blk] = own[q, me, blk].astype(BF16)

    def hop(q, t, d, up):
        to = t + 1 if up else t - 1
        came = t > 0 if up else t < last
        inbound, outbound = (up_in, up_out) if up else (down_in, down_out)
        sent, arrived = (up_send, up_recv) if up else (down_send, down_recv)
        lands = up_last if up else down_last
        land_sent, landed_sem = (up_last_send, up_last_recv) if up else (down_last_send, down_last_recv)
        if came:
            landed(arrived.at[q, d], inbound.at[q, d])
        for g in range(blks):
            value = own[q, d, g]
            if came:
                value = value + inbound[q, d, g].astype(F32)
            outbound[q, d, g] = value.astype(BF16)
        if d != to:
            pltpu.make_async_remote_copy(
                src_ref=outbound.at[q, d],
                dst_ref=inbound.at[q, d],
                send_sem=sent,
                recv_sem=arrived.at[q, d],
                device_id={"sp": to},
                device_id_type=MESH,
            ).start()
        else:
            for k in range(blks):
                g = group(k)
                pltpu.make_async_remote_copy(
                    src_ref=outbound.at[q, d, g],
                    dst_ref=lands.at[q, blk],
                    send_sem=land_sent,
                    recv_sem=landed_sem.at[q],
                    device_id={"sp": to, "blk": g},
                    device_id_type=MESH,
                ).start()

    def relay(q, t, d):
        @pl.when(me == t)
        def _():
            hop(q, t, d, True)

        @pl.when(me == last - t)
        def _():
            hop(q, last - t, last - d, False)

    def place(q, c, j):
        return pl.ds(pl.multiple_of(2 * span + (c * sp + j) * rows + q * cut, cut), cut)

    sent_cols = slice(0, pair)

    def rise(q, j):
        for c in range(blks):
            pltpu.make_async_remote_copy(
                src_ref=kv.at[place(q, c, j), sent_cols],
                dst_ref=kv.at[place(q, c, j), sent_cols],
                send_sem=rise_send,
                recv_sem=rise_recv.at[q, j],
                device_id={"sp": me + 1},
                device_id_type=MESH,
            ).start()

    def fall(q, j):
        for c in range(blks):
            pltpu.make_async_remote_copy(
                src_ref=kv.at[place(q, c, j), sent_cols],
                dst_ref=kv.at[place(q, c, j), sent_cols],
                send_sem=fall_send,
                recv_sem=fall_recv.at[q, j],
                device_id={"sp": me - 1},
                device_id_type=MESH,
            ).start()

    def close(q):
        landed(self_recv.at[q], self_in.at[q, pl.ds(0, blks - 1)])
        total[...] = self_in[q].astype(F32)

        @pl.when(me > 0)
        def _():
            landed(up_last_recv.at[q], up_last.at[q])
            total[...] = total[...] + up_last[q].astype(F32)

        @pl.when(me < last)
        def _():
            landed(down_last_recv.at[q], down_last.at[q])
            total[...] = total[...] + down_last[q].astype(F32)

        at = slice(q * cut, (q + 1) * cut)
        for c in range(blks):
            keys = total[c, :, :HEAD] + key_shift
            turned = keys * cos_buf[c, at] + pltpu.roll(keys, HEAD // 2, 1) * sin_buf[c, at]
            kv[place(q, c, me), :HEAD] = turned.astype(BF16)
            kv[place(q, c, me), HEAD:pair] = (total[c, :, HEAD:] + value_shift).astype(BF16)

        @pl.when(me < last)
        def _():
            rise(q, me)

        @pl.when(me > 0)
        def _():
            fall(q, me)

    every = kv.at[pl.ds(0, blks * cut), sent_cols]

    def gather(q, t, j):
        @pl.when(me == t)
        def _():
            landed(rise_recv.at[q, j], every)
            if t < last:
                rise(q, j)

        @pl.when(me == last - t)
        def _():
            landed(fall_recv.at[q, last - j], every)
            if t < last:
                fall(q, last - j)

    ends = []
    running = jnp.int32(0)
    for d in range(docs):
        running = running + docs_ref[d]
        ends.append(running)

    exponent = math.log2(math.e) / math.sqrt(HEAD)

    def attend(c):
        query_at = c * span + me * rows + lax.broadcasted_iota(jnp.int32, (rows, HEAD), 0)
        first = jnp.zeros((rows, HEAD), jnp.int32)
        for end in ends:
            first = jnp.where(query_at >= end, end, first)
        base = c * span + me * rows - 2 * span
        for piece in range(window // HEAD):
            key_at = base + piece * HEAD + lax.broadcasted_iota(jnp.int32, (rows, HEAD), 1)
            seen = (key_at >= first) & (key_at <= query_at)
            mask_buf[:, piece * HEAD : (piece + 1) * HEAD] = jnp.where(seen, 0.0, NEG_FILL)
        at = pl.ds(pl.multiple_of(c * span + me * rows, rows), window)
        for h in range(heads):
            cols = slice(h * HEAD, (h + 1) * HEAD)
            scores = lax.dot_general(
                qbuf[c, :, cols], kv[at, :HEAD], (((1,), (1,)), ((), ())), preferred_element_type=F32
            )
            scores = scores + mask_buf[...]
            largest = jnp.max(scores, axis=1, keepdims=True)
            weights = jnp.exp2((scores - largest) * exponent).astype(BF16)
            summed = jnp.dot(weights, kv[at, HEAD:], preferred_element_type=F32)
            obuf[c, :, cols] = (summed[:, :HEAD] / summed[:, HEAD:]).astype(BF16)

    def o_copy(c):
        return pltpu.make_async_remote_copy(
            src_ref=obuf.at[c],
            dst_ref=out_ref.at[0, :, own_cols],
            send_sem=o_send,
            recv_sem=o_recv,
            device_id={"blk": c},
            device_id_type=MESH,
        )

    def weights_in():
        for g in range(blks):
            load_w(g, 0).wait()
            load_w(g, 1).wait()

    def queries_in():
        load_q.wait()
        landed(q_recv, qbuf.at[pl.ds(0, blks - 1)])

    def finish(k, carry):
        c = group(k)
        attend(c)
        o_copy(c).start()
        return carry

    period, lag, start = 16.8 / chunks, 1.0, 12.0
    unit = period / last
    events = []
    for q in range(chunks):
        begin = start + period * q

        def first_step(q=q):
            if q == 0:
                weights_in()
            project(q)
            for d in range(last, 0, -1):
                relay(q, 0, d)
            keep(q)

        events.append((5.4 + 11.2 / chunks * (q + 1), first_step, ()))
        for t in range(1, last):
            for d in range(last, t, -1):
                arrival = begin + unit * (last - d + 1) + (t - 1) * (unit + lag) + lag
                events.append((arrival, relay, (q, t, d)))
        closed = begin + unit + (last - 1) * (unit + lag) + lag
        events.append((closed, close, (q,)))
        for j in range(last):
            free = closed
            if j == 0:
                free = max(closed, start + period * chunks + unit * q)
            for t in range(j + 1, sp):
                events.append((free + (t - j) * (unit + lag), gather, (q, t, j)))
    events.sort(key=lambda e: e[0])
    for _, step, taken in events:
        step(*taken)
    queries_in()

    lax.fori_loop(1, blks, finish, 0)
    attend(blk)
    out_ref[0, :, own_cols] = obuf[blk]

    some = pl.ds(0, blks - 1)
    left(feat_send, normed.at[:, pl.ds(0, sp - 1)])
    left(fwd_send, normed)
    left(self_send, self_out.at[:, some])
    left(q_send, qbuf.at[some])
    for t in range(sp):

        @pl.when(me == t)
        def _():
            if t < last - 1:
                left(up_send, up_out.at[:, pl.ds(0, last - t - 1)])
            if t > 1:
                left(down_send, down_out.at[:, pl.ds(0, t - 1)])
            if t < last:
                left(up_last_send, up_last)
                left(rise_send, kv.at[pl.ds(0, blks * rows * (t + 1)), sent_cols])
            if t > 0:
                left(down_last_send, down_last)
                left(fall_send, kv.at[pl.ds(0, blks * rows * (sp - t)), sent_cols])

    landed(o_recv, obuf.at[some])
    left(o_send, obuf.at[some])


CHUNKS = 4


def heads_call(operands, sp, blks, reps):
    hidden, queries, _, key_matrix = operands[:4]
    rows, width = hidden.shape[1:]
    chunks = CHUNKS
    cut = rows // chunks
    span = rows * sp
    fs, kv_cols = key_matrix.shape
    q_cols = queries.shape[2] // blks
    pair = 2 * HEAD
    vmem = pl.BlockSpec(memory_space=pltpu.VMEM)
    anywhere = pl.BlockSpec(memory_space=pl.ANY)
    smem = pl.BlockSpec(memory_space=pltpu.SMEM)
    dma = pltpu.SemaphoreType.DMA
    by_sp, each = dma((chunks, sp)), dma((chunks,))
    line = pltpu.VMEM((chunks, sp, blks, cut, pair), BF16)
    spot = pltpu.VMEM((chunks, blks, cut, pair), BF16)
    return pl.pallas_call(
        functools.partial(heads_kernel, (sp, blks, reps, rows, chunks)),
        out_shape=jax.ShapeDtypeStruct(queries.shape, BF16),
        in_specs=[anywhere, anywhere, vmem, anywhere, anywhere, vmem, vmem, smem],
        out_specs=vmem,
        scratch_shapes=[
            pltpu.VMEM((chunks, cut // reps, width), BF16),
            pltpu.VMEM((fs, 2 * kv_cols), BF16),
            pltpu.VMEM((chunks, sp, cut // reps, fs), BF16),
            pltpu.VMEM((chunks, sp, reps, cut // reps, fs), BF16),
            pltpu.VMEM((chunks, sp, blks, cut, pair), F32),
            line,
            line,
            line,
            line,
            spot,
            spot,
            spot,
            spot,
            pltpu.VMEM(((2 + blks) * span, 3 * HEAD), BF16),
            pltpu.VMEM((blks, rows, q_cols), BF16),
            pltpu.VMEM((blks, rows, q_cols), BF16),
            pltpu.VMEM((blks, cut, pair), F32),
            pltpu.VMEM((blks, rows, HEAD), F32),
            pltpu.VMEM((blks, rows, HEAD), F32),
            pltpu.VMEM((rows, 2 * span + rows), F32),
            dma((chunks + 2 * blks + 1,)),
            dma,
            by_sp,
            dma,
            each,
            dma,
            dma,
            dma,
            each,
            dma,
            by_sp,
            dma,
            each,
            dma,
            by_sp,
            dma,
            each,
            dma,
            by_sp,
            dma,
            by_sp,
            dma,
            dma,
        ],
        compiler_params=pltpu.CompilerParams(
            collective_id=0, has_side_effects=True, vmem_limit_bytes=60 * 1024 * 1024
        ),
        name="masked_attention",
    )(*operands)


def on_device(
    hidden,
    queries,
    norm_gain,
    key_matrix,
    value_matrix,
    key_shift_bias,
    value_shift_bias,
    doc_lengths,
):
    sp = lax.axis_size("sp")
    blks = lax.axis_size("blk")
    reps = lax.axis_size("rep")
    rows, width = hidden.shape[1:]
    half = rows // reps
    span = rows * sp
    fs = key_matrix.shape[0]
    kv_cols = key_matrix.shape[1]
    kv_heads = kv_cols // HEAD
    q_cols = queries.shape[2] // sp
    window = 2 * span + rows
    slots = kv_heads if sp > kv_heads else kv_heads // 2
    operands = (
        hidden,
        queries,
        norm_gain.reshape(1, width),
        key_matrix,
        value_matrix,
        key_shift_bias,
        value_shift_bias,
        doc_lengths,
    )
    if blks == kv_heads:
        return heads_call(operands, sp, blks, reps)
    vmem = pl.BlockSpec(memory_space=pltpu.VMEM)
    anywhere = pl.BlockSpec(memory_space=pl.ANY)
    smem = pl.BlockSpec(memory_space=pltpu.SMEM)
    dma = pltpu.SemaphoreType.DMA
    return pl.pallas_call(
        functools.partial(kernel, (sp, blks, reps, rows)),
        out_shape=jax.ShapeDtypeStruct(queries.shape, BF16),
        in_specs=[anywhere, anywhere, vmem, anywhere, anywhere, vmem, vmem, smem],
        out_specs=vmem,
        scratch_shapes=[
            pltpu.VMEM((half, width), BF16),
            pltpu.VMEM((fs, 2 * kv_cols), BF16),
            pltpu.VMEM((sp, half, fs), BF16),
            pltpu.VMEM((sp, reps, half, fs), BF16),
            pltpu.VMEM((kv_heads, span, 2 * HEAD), F32),
            pltpu.VMEM((kv_heads, span, 2 * HEAD), BF16),
            pltpu.VMEM((slots, span, 2 * HEAD), BF16),
            pltpu.VMEM((slots, span, 2 * HEAD), BF16),
            pltpu.VMEM((sp // 2, span, 2 * HEAD), BF16),
            pltpu.VMEM((3 * span, 2 * HEAD), BF16),
            pltpu.VMEM((sp, rows, q_cols), BF16),
            pltpu.VMEM((sp, rows, q_cols), BF16),
            pltpu.VMEM((span, HEAD), F32),
            pltpu.VMEM((span, HEAD), F32),
            pltpu.VMEM((rows, window), F32),
            dma((4,)),
            dma((sp,)),
            dma((sp,)),
            dma((sp,)),
            dma((sp,)),
            dma((sp,)),
            dma((sp,)),
            dma((slots,)),
            dma((slots, sp)),
            dma((sp // 2,)),
            dma((sp // 2, sp)),
            dma((2,)),
            dma((2, sp)),
            dma((sp,)),
            dma((sp,)),
        ],
        compiler_params=pltpu.CompilerParams(
            collective_id=0, has_side_effects=True, vmem_limit_bytes=60 * 1024 * 1024
        ),
        name="masked_attention",
    )(*operands)


def solution(mesh):
    in_specs = (
        P(("grp", "blk"), "sp", None),
        P(("grp", "blk"), "sp", "rep"),
        P(),
        P("sp", "rep"),
        P("sp", "rep"),
        P("rep"),
        P("rep"),
        P("grp"),
    )
    out_specs = P(("grp", "blk"), "sp", "rep")
    return jax.shard_map(
        on_device, mesh=mesh, in_specs=in_specs, out_specs=out_specs, check_vma=False
    )
```

```python
import functools
import math

import jax
import jax.numpy as jnp
from jax import lax
from jax.experimental import pallas as pl
from jax.experimental.pallas import tpu as pltpu
from jax.sharding import PartitionSpec as P

HEAD = 128
EPS_VALUE = 1e-06
THETA_BASE = 1000000.0
NEG_FILL = -1e30
MESH = pl.DeviceIdType.MESH
F32, BF16 = jnp.float32, jnp.bfloat16


def kernel(
    sizes,
    hidden_ref,
    queries_ref,
    gain_ref,
    kw_ref,
    vw_ref,
    kb_ref,
    vb_ref,
    docs_ref,
    out_ref,
    hid,
    wts,
    normed,
    feats,
    part_own,
    part_out,
    pair_in,
    pair_out,
    part_in,
    kv,
    qbuf,
    obuf,
    cos_buf,
    sin_buf,
    mask_buf,
    load_sem,
    feat_send,
    feat_recv,
    fwd_send,
    fwd_recv,
    q_send,
    q_recv,
    pair_send,
    pair_recv,
    part_send,
    part_recv,
    kv_send,
    kv_recv,
    o_send,
    o_recv,
):
    sp, blks, reps, rows = sizes
    me = lax.axis_index("sp")
    blk = lax.axis_index("blk")
    rep = lax.axis_index("rep")
    half = rows // reps
    span = sp * rows
    fs = kw_ref.shape[0]
    kv_heads = kw_ref.shape[1] // HEAD
    fold = sp // kv_heads
    my_head = me // fold
    q_cols = queries_ref.shape[2] // sp
    heads = q_cols // HEAD
    window = 2 * span + rows
    docs = docs_ref.shape[0]

    pairs = sp // 2
    my_pair = me // 2
    parity = lax.rem(me, 2)
    slots = pair_in.shape[0]

    def place(k):
        pair = lax.rem(my_pair + k // 2, pairs)
        return 2 * pair + lax.rem(parity + lax.rem(k, 2), 2)

    peer = place
    partner = place(1)

    def slot_head(slot, side):
        return slot if fold > 1 else 2 * slot + side

    barrier = pltpu.get_barrier_semaphore()
    for k in range(1, sp):
        pl.semaphore_signal(barrier, inc=1, device_id={"sp": peer(k)}, device_id_type=MESH)
    for k in range(1, reps):
        pl.semaphore_signal(
            barrier, inc=1, device_id={"rep": lax.rem(rep + k, reps)}, device_id_type=MESH
        )
    for dist in (1, 2):
        pl.semaphore_signal(
            barrier, inc=1, device_id={"blk": lax.rem(blk + dist, blks)}, device_id_type=MESH
        )
        pl.semaphore_signal(
            barrier, inc=1, device_id={"blk": lax.rem(blk + blks - dist, blks)}, device_id_type=MESH
        )

    load_hid = pltpu.make_async_copy(
        hidden_ref.at[0, pl.ds(pl.multiple_of(rep * half, half), half)], hid, load_sem.at[0]
    )
    load_k = pltpu.make_async_copy(kw_ref, wts.at[:, : kv_heads * HEAD], load_sem.at[1])
    load_v = pltpu.make_async_copy(vw_ref, wts.at[:, kv_heads * HEAD :], load_sem.at[2])
    load_q = pltpu.make_async_copy(
        queries_ref.at[0, :, pl.ds(pl.multiple_of(me * q_cols, q_cols), q_cols)],
        qbuf.at[me],
        load_sem.at[3],
    )
    load_hid.start()
    load_k.start()
    load_v.start()
    load_q.start()

    load_hid.wait()
    values = hid[...].astype(F32)
    scale = lax.rsqrt(jnp.mean(values * values, axis=1, keepdims=True) + EPS_VALUE)
    for d in range(sp):
        cols = slice(d * fs, (d + 1) * fs)
        normed[d] = (hid[:, cols].astype(F32) * scale * gain_ref[:, cols]).astype(BF16)

    pl.semaphore_wait(barrier, sp - 1 + reps - 1 + 4)

    def feat_copy(k):
        d = peer(k)
        return pltpu.make_async_remote_copy(
            src_ref=normed.at[d],
            dst_ref=feats.at[me, rep],
            send_sem=feat_send.at[d],
            recv_sem=feat_recv.at[me],
            device_id={"sp": d},
            device_id_type=MESH,
        )

    def feat_arrival(s):
        return pltpu.make_async_remote_copy(
            src_ref=normed.at[0],
            dst_ref=feats.at[s, rep],
            send_sem=feat_send.at[0],
            recv_sem=feat_recv.at[s],
            device_id={"sp": s},
            device_id_type=MESH,
        )

    other = lax.rem(rep + 1, reps)

    def fwd_copy(s, source):
        return pltpu.make_async_remote_copy(
            src_ref=source,
            dst_ref=feats.at[s, rep],
            send_sem=fwd_send.at[s],
            recv_sem=fwd_recv.at[s],
            device_id={"rep": other},
            device_id_type=MESH,
        )

    def fwd_arrival(s):
        return pltpu.make_async_remote_copy(
            src_ref=normed.at[0],
            dst_ref=feats.at[s, other],
            send_sem=fwd_send.at[s],
            recv_sem=fwd_recv.at[s],
            device_id={"rep": other},
            device_id_type=MESH,
        )

    order = list(range(1, sp))
    for k in order:
        feat_copy(k).start()
    fwd_copy(me, normed.at[me]).start()
    feats[me, rep] = normed[me]

    token_base = blk * span
    lanes = lax.broadcasted_iota(jnp.int32, (1, HEAD), 1)
    index = lax.rem(lanes, HEAD // 2).astype(F32)
    inverse = jnp.exp(index * (-2.0 * math.log(THETA_BASE) / HEAD))
    sign = jnp.where(lanes < HEAD // 2, -1.0, 1.0)

    def angle_step(j, carry):
        at = pl.ds(pl.multiple_of(j * rows, rows), rows)
        places = token_base + j * rows + lax.broadcasted_iota(jnp.int32, (rows, HEAD), 0)
        angles = places.astype(F32) * inverse
        cos_buf[at, :] = jnp.cos(angles)
        sin_buf[at, :] = jnp.sin(angles) * sign
        return carry

    lax.fori_loop(0, sp, angle_step, 0)
    load_k.wait()
    load_v.wait()

    def rows_of(j):
        return pl.ds(pl.multiple_of(j * rows, rows), rows)

    def pair_copy(slot, j):
        return pltpu.make_async_remote_copy(
            src_ref=part_out.at[slot_head(slot, 1 - parity), rows_of(j)],
            dst_ref=pair_in.at[slot, rows_of(j)],
            send_sem=pair_send.at[slot],
            recv_sem=pair_recv.at[slot, j],
            device_id={"sp": partner},
            device_id_type=MESH,
        )

    def part_copy(d, j):
        slot = d // fold if fold > 1 else d // 2
        return pltpu.make_async_remote_copy(
            src_ref=pair_out.at[slot, rows_of(j)],
            dst_ref=part_in.at[my_pair, rows_of(j)],
            send_sem=part_send.at[d // 2],
            recv_sem=part_recv.at[my_pair, j],
            device_id={"sp": d},
            device_id_type=MESH,
        )

    def far(k):
        return 2 * lax.rem(my_pair + k, pairs) + parity

    def project(j):
        at = rows_of(j)
        block = feats[j].reshape(rows, fs)
        partial = jnp.dot(block, wts[...], preferred_element_type=F32)
        for h in range(kv_heads):
            key_part = partial[:, h * HEAD : (h + 1) * HEAD]
            value_part = partial[:, (kv_heads + h) * HEAD : (kv_heads + h + 1) * HEAD]
            part_own[h, at, :HEAD] = key_part
            part_own[h, at, HEAD:] = value_part
            part_out[h, at, :HEAD] = key_part.astype(BF16)
            part_out[h, at, HEAD:] = value_part.astype(BF16)
        for slot in range(slots):
            pair_copy(slot, j).start()

    def cross(j):
        at = rows_of(j)
        for slot in range(slots):
            pair_copy(slot, j).wait_recv()
            both = part_own[slot_head(slot, parity), at, :] + pair_in[slot, at, :].astype(F32)
            part_own[slot_head(slot, parity), at, :] = both
            pair_out[slot, at, :] = both.astype(BF16)
        for k in range(1, pairs):
            part_copy(far(k), j).start()

    fwd_arrival(me).wait_recv()
    project(me)

    def arrive(k, carry):
        s = place(k)
        feat_arrival(s).wait_recv()
        fwd_copy(s, feats.at[s, rep]).start()
        fwd_arrival(s).wait_recv()
        project(s)
        cross(place(k - 1))
        return carry

    lax.fori_loop(1, sp, arrive, 0)
    cross(place(sp - 1))

    def q_copy(d):
        return pltpu.make_async_remote_copy(
            src_ref=queries_ref.at[0, :, pl.ds(pl.multiple_of(d * q_cols, q_cols), q_cols)],
            dst_ref=qbuf.at[me],
            send_sem=q_send.at[d],
            recv_sem=q_recv.at[me],
            device_id={"sp": d},
            device_id_type=MESH,
        )

    def q_arrival(s):
        return pltpu.make_async_remote_copy(
            src_ref=qbuf.at[s],
            dst_ref=qbuf.at[s],
            send_sem=q_send.at[s],
            recv_sem=q_recv.at[s],
            device_id={"sp": s},
            device_id_type=MESH,
        )

    for k in reversed(order):
        q_copy(peer(k)).start()

    for piece in (0, 1):

        @pl.when(blk < 2 - piece)
        def _():
            kv[pl.ds(piece * span, span), :] = jnp.zeros((span, 2 * HEAD), BF16)


    def own_shift(ref):
        row = ref[...].astype(F32).reshape(1, kv_heads * HEAD)
        mine = row[:, :HEAD]
        for h in range(1, kv_heads):
            mine = jnp.where(my_head == h, row[:, h * HEAD : (h + 1) * HEAD], mine)
        return mine

    key_shift = own_shift(kb_ref)
    value_shift = own_shift(vb_ref)

    relay = blks == 4

    def kv_copy(piece, dist, j):
        return pltpu.make_async_remote_copy(
            src_ref=kv.at[pl.ds(pl.multiple_of(piece * span + j * rows, rows), rows)],
            dst_ref=kv.at[pl.ds(pl.multiple_of((2 - dist) * span + j * rows, rows), rows)],
            send_sem=kv_send.at[dist - 1],
            recv_sem=kv_recv.at[dist - 1, j],
            device_id={"blk": lax.rem(blk + dist, blks)},
            device_id_type=MESH,
        )

    def kv_pass(j):
        kv_copy(2, 2, j).wait_recv()
        pltpu.make_async_remote_copy(
            src_ref=kv.at[pl.ds(pl.multiple_of(j * rows, rows), rows)],
            dst_ref=kv.at[pl.ds(pl.multiple_of(span + j * rows, rows), rows)],
            send_sem=kv_send.at[0],
            recv_sem=kv_recv.at[0, j],
            device_id={"blk": lax.rem(blk + blks - 1, blks)},
            device_id_type=MESH,
        ).start()

    near = blk + 1 < blks
    if relay:
        near = near & (blk != 1)
    sends = {1: near, 2: blk + 2 < blks}

    def finish(i, carry):
        j = place(i)
        at = rows_of(j)
        total = part_own[my_head, at, :]
        for k in range(1, pairs):
            s = lax.rem(my_pair + k, pairs)
            pltpu.make_async_remote_copy(
                src_ref=part_in.at[s, at],
                dst_ref=part_in.at[s, at],
                send_sem=part_send.at[s],
                recv_sem=part_recv.at[s, j],
                device_id={"sp": far(k)},
                device_id_type=MESH,
            ).wait_recv()
            total = total + part_in[s, at, :].astype(F32)
        keys = total[:, :HEAD] + key_shift
        turned = keys * cos_buf[at, :] + pltpu.roll(keys, HEAD // 2, 1) * sin_buf[at, :]
        put = pl.ds(pl.multiple_of(2 * span + j * rows, rows), rows)
        kv[put, :HEAD] = turned.astype(BF16)
        kv[put, HEAD:] = (total[:, HEAD:] + value_shift).astype(BF16)
        for dist in (2, 1):

            @pl.when(sends[dist])
            def _():
                kv_copy(2, dist, j).start()

        if relay:

            @pl.when((blk == 3) & (i >= 1))
            def _():
                kv_pass(place(i - 1))

        return carry

    lax.fori_loop(0, sp, finish, 0)
    if relay:

        @pl.when(blk == 3)
        def _():
            kv_pass(place(sp - 1))


    ends = []
    running = jnp.int32(0)
    for d in range(docs):
        running = running + docs_ref[d]
        ends.append(running)

    load_q.wait()
    for dist in (1, 2):

        arrives = blk >= dist
        if relay and dist == 2:
            arrives = arrives & (blk != 3)

        @pl.when(arrives)
        def _():
            for j in range(sp):
                kv_copy(2, dist, j).wait_recv()

    exponent = math.log2(math.e) / math.sqrt(HEAD)

    def attend(t):
        query_at = token_base + t * rows + lax.broadcasted_iota(jnp.int32, (rows, HEAD), 0)
        first = jnp.zeros((rows, HEAD), jnp.int32)
        for end in ends:
            first = jnp.where(query_at >= end, end, first)
        key_base = token_base - 2 * span + t * rows
        for c in range(window // HEAD):
            key_at = key_base + c * HEAD + lax.broadcasted_iota(jnp.int32, (rows, HEAD), 1)
            seen = (key_at >= first) & (key_at <= query_at)
            mask_buf[:, c * HEAD : (c + 1) * HEAD] = jnp.where(seen, 0.0, NEG_FILL)
        at = pl.ds(pl.multiple_of(t * rows, rows), window)
        for h in range(heads):
            cols = slice(h * HEAD, (h + 1) * HEAD)
            scores = lax.dot_general(
                qbuf[t, :, cols], kv[at, :HEAD], (((1,), (1,)), ((), ())), preferred_element_type=F32
            )
            scores = scores + mask_buf[...]
            largest = jnp.max(scores, axis=1, keepdims=True)
            weights = jnp.exp2((scores - largest) * exponent).astype(BF16)
            total = jnp.sum(weights.astype(F32), axis=1, keepdims=True)
            summed = jnp.dot(weights, kv[at, HEAD:], preferred_element_type=F32)
            obuf[t, :, cols] = (summed / total).astype(BF16)

    my_cols = pl.ds(pl.multiple_of(me * q_cols, q_cols), q_cols)

    def o_copy(d):
        return pltpu.make_async_remote_copy(
            src_ref=obuf.at[d],
            dst_ref=out_ref.at[0, :, my_cols],
            send_sem=o_send.at[d],
            recv_sem=o_recv.at[me],
            device_id={"sp": d},
            device_id_type=MESH,
        )

    def o_arrival(s):
        return pltpu.make_async_remote_copy(
            src_ref=obuf.at[s],
            dst_ref=out_ref.at[0, :, pl.ds(pl.multiple_of(s * q_cols, q_cols), q_cols)],
            send_sem=o_send.at[s],
            recv_sem=o_recv.at[s],
            device_id={"sp": s},
            device_id_type=MESH,
        )

    def each(k, carry):
        t = place(sp - k)
        q_arrival(t).wait_recv()
        attend(t)
        o_copy(t).start()
        return carry

    lax.fori_loop(1, sp, each, 0)
    attend(me)
    out_ref[0, :, my_cols] = obuf[me]

    for k in order:
        d = peer(k)
        o_arrival(d).wait_recv()
        o_copy(d).wait_send()
        feat_copy(k).wait_send()
        q_copy(d).wait_send()
        fwd_copy(d, feats.at[d, rep]).wait_send()
    fwd_copy(me, normed.at[me]).wait_send()

    def sent(sem, source):
        pltpu.make_async_remote_copy(
            src_ref=source,
            dst_ref=source,
            send_sem=sem,
            recv_sem=part_recv.at[0, 0],
            device_id={"sp": partner},
            device_id_type=MESH,
        ).wait_send()

    for slot in range(slots):
        sent(pair_send.at[slot], pair_in.at[slot])
    for k in range(1, pairs):
        sent(part_send.at[far(k) // 2], part_in.at[0])
    for dist in (1, 2):

        shipped = sends[dist]
        if relay and dist == 1:
            shipped = shipped | (blk == 3)

        @pl.when(shipped)
        def _():
            sent(kv_send.at[dist - 1], kv.at[pl.ds(0, span)])


def heads_kernel(
    sizes,
    hidden_ref,
    queries_ref,
    gain_ref,
    kw_ref,
    vw_ref,
    kb_ref,
    vb_ref,
    docs_ref,
    out_ref,
    hid,
    wts,
    normed,
    feats,
    own,
    up_in,
    up_out,
    down_in,
    down_out,
    self_out,
    self_in,
    up_last,
    down_last,
    kv,
    qbuf,
    obuf,
    total,
    cos_buf,
    sin_buf,
    mask_buf,
    load_sem,
    feat_send,
    feat_recv,
    fwd_send,
    fwd_recv,
    q_send,
    q_recv,
    self_send,
    self_recv,
    up_send,
    up_recv,
    up_last_send,
    up_last_recv,
    down_send,
    down_recv,
    down_last_send,
    down_last_recv,
    rise_send,
    rise_recv,
    fall_send,
    fall_recv,
    o_send,
    o_recv,
):
    sp, blks, reps, rows, chunks = sizes
    me = lax.axis_index("sp")
    blk = lax.axis_index("blk")
    rep = lax.axis_index("rep")
    span = sp * rows
    cut = rows // chunks
    part = cut // reps
    fs = kw_ref.shape[0]
    q_cols = queries_ref.shape[2] // blks
    heads = q_cols // HEAD
    docs = docs_ref.shape[0]
    window = 2 * span + rows
    last = sp - 1
    pair = 2 * HEAD

    turn = 2 * lax.rem(blk, 2) - 1

    def group(k):
        return lax.rem(blk + blks + k * turn, blks)

    barrier = pltpu.get_barrier_semaphore()
    for k in range(1, sp):
        pl.semaphore_signal(
            barrier, inc=1, device_id={"sp": lax.rem(me + k, sp)}, device_id_type=MESH
        )
    for k in range(1, reps):
        pl.semaphore_signal(
            barrier, inc=1, device_id={"rep": lax.rem(rep + k, reps)}, device_id_type=MESH
        )
    for k in range(1, blks):
        pl.semaphore_signal(barrier, inc=1, device_id={"blk": group(k)}, device_id_type=MESH)

        @pl.when(me > 0)
        def _():
            pl.semaphore_signal(
                barrier, inc=1, device_id={"sp": me - 1, "blk": group(k)}, device_id_type=MESH
            )

        @pl.when(me < last)
        def _():
            pl.semaphore_signal(
                barrier, inc=1, device_id={"sp": me + 1, "blk": group(k)}, device_id_type=MESH
            )

    def load_hid(q):
        return pltpu.make_async_copy(
            hidden_ref.at[0, pl.ds(pl.multiple_of(q * cut + rep * part, part), part)],
            hid.at[q],
            load_sem.at[q],
        )

    def load_w(g, side):
        source = vw_ref if side else kw_ref
        return pltpu.make_async_copy(
            source.at[:, g * HEAD : (g + 1) * HEAD],
            wts.at[:, (2 * g + side) * HEAD : (2 * g + side + 1) * HEAD],
            load_sem.at[chunks + 2 * g + side],
        )

    own_cols = pl.ds(pl.multiple_of(blk * q_cols, q_cols), q_cols)
    load_q = pltpu.make_async_copy(
        queries_ref.at[0, :, own_cols], qbuf.at[blk], load_sem.at[chunks + 2 * blks]
    )
    for q in range(chunks):
        load_hid(q).start()
    for g in range(blks):
        load_w(g, 0).start()
        load_w(g, 1).start()
    load_q.start()

    def feat_copy(q, d):
        return pltpu.make_async_remote_copy(
            src_ref=normed.at[q, d],
            dst_ref=feats.at[q, me, rep],
            send_sem=feat_send,
            recv_sem=feat_recv.at[q, me],
            device_id={"sp": d},
            device_id_type=MESH,
        )

    def feat_arrival(q, s):
        return pltpu.make_async_remote_copy(
            src_ref=normed.at[q, 0],
            dst_ref=feats.at[q, s, rep],
            send_sem=feat_send,
            recv_sem=feat_recv.at[q, s],
            device_id={"sp": s},
            device_id_type=MESH,
        )

    other = lax.rem(rep + 1, reps)

    def fwd_copy(q, s, source):
        return pltpu.make_async_remote_copy(
            src_ref=source,
            dst_ref=feats.at[q, s, rep],
            send_sem=fwd_send,
            recv_sem=fwd_recv.at[q],
            device_id={"rep": other},
            device_id_type=MESH,
        )

    def q_copy(g):
        return pltpu.make_async_remote_copy(
            src_ref=queries_ref.at[0, :, pl.ds(pl.multiple_of(g * q_cols, q_cols), q_cols)],
            dst_ref=qbuf.at[blk],
            send_sem=q_send,
            recv_sem=q_recv,
            device_id={"blk": g},
            device_id_type=MESH,
        )

    def norm(q):
        load_hid(q).wait()
        values = hid[q].astype(F32)
        scale = lax.rsqrt(jnp.mean(values * values, axis=1, keepdims=True) + EPS_VALUE)
        for d in range(sp):
            cols = slice(d * fs, (d + 1) * fs)
            normed[q, d] = (hid[q, :, cols].astype(F32) * scale * gain_ref[:, cols]).astype(BF16)

    norm(0)
    peers = sp - 1 + reps - 1 + blks - 1

    @pl.when((me == 0) | (me == last))
    def _():
        pl.semaphore_wait(barrier, peers + blks - 1)

    @pl.when((me > 0) & (me < last))
    def _():
        pl.semaphore_wait(barrier, peers + 2 * (blks - 1))

    for q in range(chunks):
        if q > 0:
            norm(q)
        for step in range(1, sp):
            far = jnp.where(rep == 0, step, sp - step)

            @pl.when(me + far < sp)
            def _():
                feat_copy(q, me + far).start()

            @pl.when(me >= far)
            def _():
                feat_copy(q, me - far).start()

        fwd_copy(q, me, normed.at[q, me]).start()
        feats[q, me, rep] = normed[q, me]
    for k in range(1, blks):
        q_copy(group(k)).start()

    lanes = lax.broadcasted_iota(jnp.int32, (1, HEAD), 1)
    index = lax.rem(lanes, HEAD // 2).astype(F32)
    inverse = jnp.exp(index * (-2.0 * math.log(THETA_BASE) / HEAD))
    sign = jnp.where(lanes < HEAD // 2, -1.0, 1.0)

    def angle_step(c, carry):
        places = c * span + me * rows + lax.broadcasted_iota(jnp.int32, (rows, HEAD), 0)
        angles = places.astype(F32) * inverse
        cos_buf[c] = jnp.cos(angles)
        sin_buf[c] = jnp.sin(angles) * sign
        return carry

    lax.fori_loop(0, blks, angle_step, 0)
    kv[: 2 * span, :pair] = jnp.zeros((2 * span, pair), BF16)
    kv[:, pair:] = jnp.ones((kv.shape[0], HEAD), BF16)

    def own_shift(ref):
        row = ref[...].astype(F32).reshape(1, blks * HEAD)
        mine = row[:, :HEAD]
        for g in range(1, blks):
            mine = jnp.where(blk == g, row[:, g * HEAD : (g + 1) * HEAD], mine)
        return mine

    key_shift = own_shift(kb_ref)
    value_shift = own_shift(vb_ref)

    def landed(sem, ref):
        pltpu.make_async_remote_copy(
            src_ref=ref,
            dst_ref=ref,
            send_sem=sem,
            recv_sem=sem,
            device_id={"rep": other},
            device_id_type=MESH,
        ).wait_recv()

    def left(sem, ref):
        pltpu.make_async_remote_copy(
            src_ref=ref,
            dst_ref=ref,
            send_sem=sem,
            recv_sem=sem,
            device_id={"rep": other},
            device_id_type=MESH,
        ).wait_send()

    def self_copy(q, g):
        return pltpu.make_async_remote_copy(
            src_ref=self_out.at[q, g],
            dst_ref=self_in.at[q, blk],
            send_sem=self_send,
            recv_sem=self_recv.at[q],
            device_id={"blk": g},
            device_id_type=MESH,
        )

    def project(q):
        for far in range(1, sp):

            @pl.when(me >= far)
            def _():
                feat_arrival(q, me - far).wait_recv()
                fwd_copy(q, me - far, feats.at[q, me - far, rep]).start()

            @pl.when(me + far < sp)
            def _():
                feat_arrival(q, me + far).wait_recv()
                fwd_copy(q, me + far, feats.at[q, me + far, rep]).start()

        landed(fwd_recv.at[q], normed.at[q])
        partial = jnp.dot(
            feats[q].reshape(sp * cut, fs), wts[...], preferred_element_type=F32
        )
        for j in range(sp):
            for g in range(blks):
                own[q, j, g] = partial[j * cut : (j + 1) * cut, g * pair : (g + 1) * pair]

    def keep(q):
        for k in range(1, blks):
            g = group(k)
            self_out[q, g] = own[q, me, g].astype(BF16)
            self_copy(q, g).start()
        self_in[q, blk] = own[q, me, blk].astype(BF16)

    def hop(q, t, d, up):
        to = t + 1 if up else t - 1
        came = t > 0 if up else t < last
        inbound, outbound = (up_in, up_out) if up else (down_in, down_out)
        sent, arrived = (up_send, up_recv) if up else (down_send, down_recv)
        lands = up_last if up else down_last
        land_sent, landed_sem = (up_last_send, up_last_recv) if up else (down_last_send, down_last_recv)
        if came:
            landed(arrived.at[q, d], inbound.at[q, d])
        for g in range(blks):
            value = own[q, d, g]
            if came:
                value = value + inbound[q, d, g].astype(F32)
            outbound[q, d, g] = value.astype(BF16)
        if d != to:
            pltpu.make_async_remote_copy(
                src_ref=outbound.at[q, d],
                dst_ref=inbound.at[q, d],
                send_sem=sent,
                recv_sem=arrived.at[q, d],
                device_id={"sp": to},
                device_id_type=MESH,
            ).start()
        else:
            for k in range(blks):
                g = group(k)
                pltpu.make_async_remote_copy(
                    src_ref=outbound.at[q, d, g],
                    dst_ref=lands.at[q, blk],
                    send_sem=land_sent,
                    recv_sem=landed_sem.at[q],
                    device_id={"sp": to, "blk": g},
                    device_id_type=MESH,
                ).start()

    def relay(q, t, d):
        @pl.when(me == t)
        def _():
            hop(q, t, d, True)

        @pl.when(me == last - t)
        def _():
            hop(q, last - t, last - d, False)

    def place(q, c, j):
        return pl.ds(pl.multiple_of(2 * span + (c * sp + j) * rows + q * cut, cut), cut)

    sent_cols = slice(0, pair)

    def rise(q, j):
        for c in range(blks):
            pltpu.make_async_remote_copy(
                src_ref=kv.at[place(q, c, j), sent_cols],
                dst_ref=kv.at[place(q, c, j), sent_cols],
                send_sem=rise_send,
                recv_sem=rise_recv.at[q, j],
                device_id={"sp": me + 1},
                device_id_type=MESH,
            ).start()

    def fall(q, j):
        for c in range(blks):
            pltpu.make_async_remote_copy(
                src_ref=kv.at[place(q, c, j), sent_cols],
                dst_ref=kv.at[place(q, c, j), sent_cols],
                send_sem=fall_send,
                recv_sem=fall_recv.at[q, j],
                device_id={"sp": me - 1},
                device_id_type=MESH,
            ).start()

    def close(q):
        landed(self_recv.at[q], self_in.at[q, pl.ds(0, blks - 1)])
        total[...] = self_in[q].astype(F32)

        @pl.when(me > 0)
        def _():
            landed(up_last_recv.at[q], up_last.at[q])
            total[...] = total[...] + up_last[q].astype(F32)

        @pl.when(me < last)
        def _():
            landed(down_last_recv.at[q], down_last.at[q])
            total[...] = total[...] + down_last[q].astype(F32)

        at = slice(q * cut, (q + 1) * cut)
        for c in range(blks):
            keys = total[c, :, :HEAD] + key_shift
            turned = keys * cos_buf[c, at] + pltpu.roll(keys, HEAD // 2, 1) * sin_buf[c, at]
            kv[place(q, c, me), :HEAD] = turned.astype(BF16)
            kv[place(q, c, me), HEAD:pair] = (total[c, :, HEAD:] + value_shift).astype(BF16)

        @pl.when(me < last)
        def _():
            rise(q, me)

        @pl.when(me > 0)
        def _():
            fall(q, me)

    def close_inner(q):
        @pl.when((me > 0) & (me < last))
        def _():
            close(q)

    def close_outer(q):
        @pl.when((me == 0) | (me == last))
        def _():
            close(q)

    every = kv.at[pl.ds(0, blks * cut), sent_cols]

    def gather(q, t, j):
        @pl.when(me == t)
        def _():
            landed(rise_recv.at[q, j], every)
            if t < last:
                rise(q, j)

        @pl.when(me == last - t)
        def _():
            landed(fall_recv.at[q, last - j], every)
            if t < last:
                fall(q, last - j)

    ends = []
    running = jnp.int32(0)
    for d in range(docs):
        running = running + docs_ref[d]
        ends.append(running)

    exponent = math.log2(math.e) / math.sqrt(HEAD)

    def attend(c):
        query_at = c * span + me * rows + lax.broadcasted_iota(jnp.int32, (rows, HEAD), 0)
        first = jnp.zeros((rows, HEAD), jnp.int32)
        for end in ends:
            first = jnp.where(query_at >= end, end, first)
        base = c * span + me * rows - 2 * span
        for piece in range(window // HEAD):
            key_at = base + piece * HEAD + lax.broadcasted_iota(jnp.int32, (rows, HEAD), 1)
            seen = (key_at >= first) & (key_at <= query_at)
            mask_buf[:, piece * HEAD : (piece + 1) * HEAD] = jnp.where(seen, 0.0, NEG_FILL)
        at = pl.ds(pl.multiple_of(c * span + me * rows, rows), window)
        for h in range(heads):
            cols = slice(h * HEAD, (h + 1) * HEAD)
            scores = lax.dot_general(
                qbuf[c, :, cols], kv[at, :HEAD], (((1,), (1,)), ((), ())), preferred_element_type=F32
            )
            scores = scores + mask_buf[...]
            largest = jnp.max(scores, axis=1, keepdims=True)
            weights = jnp.exp2((scores - largest) * exponent).astype(BF16)
            summed = jnp.dot(weights, kv[at, HEAD:], preferred_element_type=F32)
            obuf[c, :, cols] = (summed[:, :HEAD] / summed[:, HEAD:]).astype(BF16)

    def o_copy(c):
        return pltpu.make_async_remote_copy(
            src_ref=obuf.at[c],
            dst_ref=out_ref.at[0, :, own_cols],
            send_sem=o_send,
            recv_sem=o_recv,
            device_id={"blk": c},
            device_id_type=MESH,
        )

    def weights_in():
        for g in range(blks):
            load_w(g, 0).wait()
            load_w(g, 1).wait()

    def queries_in():
        load_q.wait()
        landed(q_recv, qbuf.at[pl.ds(0, blks - 1)])

    def finish(k, carry):
        attend(group(k))
        o_copy(group(k)).start()
        return carry

    unit, hop_time, lead = 5.6 / chunks, 3.3, 12.0
    inner_late, outer_late, gather_late, first_late = 1.0, 0.0, 1.5, 0.0
    hold = 0
    feed_first, feed_step = 10.0, 11.2 / chunks
    queue = []
    for q in range(chunks + hold):
        if q < chunks:
            queue.append((q, last))
        if q >= hold and hold:
            queue.append((q - hold, 1))
        if q < chunks:
            queue.extend((q, d) for d in range(last - 1, 0 if not hold else 1, -1))
    came = {item: lead + unit * (n + 1) + 1.0 for n, item in enumerate(queue)}
    fed = lead + unit * len(queue) + 1.0
    events = []
    for q in range(chunks):

        def first_step(q=q):
            if q == 0:
                weights_in()
            project(q)
            begin = queue.index((q, last))
            end = queue.index((q + 1, last)) if q + 1 < chunks else len(queue)
            for n in range(begin, end):
                relay(queue[n][0], 0, queue[n][1])
            keep(q)

        events.append((feed_first + feed_step * q, first_step, ()))
        for t in range(1, last):
            for d in range(last, t, -1):
                events.append((came[q, d] + hop_time * (t - 1), relay, (q, t, d)))
        inner = max(came[q, 1], came[q, last - 1] + hop_time) + inner_late
        outer = came[q, last] + hop_time * (last - 1) + outer_late
        events.append((inner, close_inner, (q,)))
        events.append((outer, close_outer, (q,)))
        for j in range(last):
            for t in range(j + 1, sp):
                if j == 0:
                    come = max(outer + hop_time, fed + unit * (q + 1)) + first_late
                else:
                    come = inner + hop_time + gather_late
                when = come + (t - j - 1) * hop_time
                events.append((1000.0 + when if t == last else when, gather, (q, t, j)))
    events.sort(key=lambda e: e[0])
    for _, step, taken in events:
        step(*taken)
    queries_in()

    lax.fori_loop(1, blks, finish, 0)
    attend(blk)
    out_ref[0, :, own_cols] = obuf[blk]

    some = pl.ds(0, blks - 1)
    left(feat_send, normed.at[:, pl.ds(0, sp - 1)])
    left(fwd_send, normed)
    left(self_send, self_out.at[:, some])
    left(q_send, qbuf.at[some])
    for t in range(sp):

        @pl.when(me == t)
        def _():
            if t < last - 1:
                left(up_send, up_out.at[:, pl.ds(0, last - t - 1)])
            if t > 1:
                left(down_send, down_out.at[:, pl.ds(0, t - 1)])
            if t < last:
                left(up_last_send, up_last)
                left(rise_send, kv.at[pl.ds(0, blks * rows * (t + 1)), sent_cols])
            if t > 0:
                left(down_last_send, down_last)
                left(fall_send, kv.at[pl.ds(0, blks * rows * (sp - t)), sent_cols])

    landed(o_recv, obuf.at[some])
    left(o_send, obuf.at[some])


CHUNKS = 4


def heads_call(operands, sp, blks, reps):
    hidden, queries, _, key_matrix = operands[:4]
    rows, width = hidden.shape[1:]
    chunks = CHUNKS
    cut = rows // chunks
    span = rows * sp
    fs, kv_cols = key_matrix.shape
    q_cols = queries.shape[2] // blks
    pair = 2 * HEAD
    vmem = pl.BlockSpec(memory_space=pltpu.VMEM)
    anywhere = pl.BlockSpec(memory_space=pl.ANY)
    smem = pl.BlockSpec(memory_space=pltpu.SMEM)
    dma = pltpu.SemaphoreType.DMA
    by_sp, each = dma((chunks, sp)), dma((chunks,))
    line = pltpu.VMEM((chunks, sp, blks, cut, pair), BF16)
    spot = pltpu.VMEM((chunks, blks, cut, pair), BF16)
    return pl.pallas_call(
        functools.partial(heads_kernel, (sp, blks, reps, rows, chunks)),
        out_shape=pltpu.VMEM(queries.shape, BF16),
        in_specs=[anywhere, anywhere, vmem, anywhere, anywhere, vmem, vmem, smem],
        out_specs=vmem,
        scratch_shapes=[
            pltpu.VMEM((chunks, cut // reps, width), BF16),
            pltpu.VMEM((fs, 2 * kv_cols), BF16),
            pltpu.VMEM((chunks, sp, cut // reps, fs), BF16),
            pltpu.VMEM((chunks, sp, reps, cut // reps, fs), BF16),
            pltpu.VMEM((chunks, sp, blks, cut, pair), F32),
            line,
            line,
            line,
            line,
            spot,
            spot,
            spot,
            spot,
            pltpu.VMEM(((2 + blks) * span, 3 * HEAD), BF16),
            pltpu.VMEM((blks, rows, q_cols), BF16),
            pltpu.VMEM((blks, rows, q_cols), BF16),
            pltpu.VMEM((blks, cut, pair), F32),
            pltpu.VMEM((blks, rows, HEAD), F32),
            pltpu.VMEM((blks, rows, HEAD), F32),
            pltpu.VMEM((rows, 2 * span + rows), F32),
            dma((chunks + 2 * blks + 1,)),
            dma,
            by_sp,
            dma,
            each,
            dma,
            dma,
            dma,
            each,
            dma,
            by_sp,
            dma,
            each,
            dma,
            by_sp,
            dma,
            each,
            dma,
            by_sp,
            dma,
            by_sp,
            dma,
            dma,
        ],
        compiler_params=pltpu.CompilerParams(
            collective_id=0, has_side_effects=True, vmem_limit_bytes=60 * 1024 * 1024
        ),
        name="masked_attention",
    )(*operands)


def on_device(
    hidden,
    queries,
    norm_gain,
    key_matrix,
    value_matrix,
    key_shift_bias,
    value_shift_bias,
    doc_lengths,
):
    sp = lax.axis_size("sp")
    blks = lax.axis_size("blk")
    reps = lax.axis_size("rep")
    rows, width = hidden.shape[1:]
    half = rows // reps
    span = rows * sp
    fs = key_matrix.shape[0]
    kv_cols = key_matrix.shape[1]
    kv_heads = kv_cols // HEAD
    q_cols = queries.shape[2] // sp
    window = 2 * span + rows
    slots = kv_heads if sp > kv_heads else kv_heads // 2
    operands = (
        hidden,
        queries,
        norm_gain.reshape(1, width),
        key_matrix,
        value_matrix,
        key_shift_bias,
        value_shift_bias,
        doc_lengths,
    )
    if blks == kv_heads:
        return heads_call(operands, sp, blks, reps)
    vmem = pl.BlockSpec(memory_space=pltpu.VMEM)
    anywhere = pl.BlockSpec(memory_space=pl.ANY)
    smem = pl.BlockSpec(memory_space=pltpu.SMEM)
    dma = pltpu.SemaphoreType.DMA
    return pl.pallas_call(
        functools.partial(kernel, (sp, blks, reps, rows)),
        out_shape=jax.ShapeDtypeStruct(queries.shape, BF16),
        in_specs=[anywhere, anywhere, vmem, anywhere, anywhere, vmem, vmem, smem],
        out_specs=vmem,
        scratch_shapes=[
            pltpu.VMEM((half, width), BF16),
            pltpu.VMEM((fs, 2 * kv_cols), BF16),
            pltpu.VMEM((sp, half, fs), BF16),
            pltpu.VMEM((sp, reps, half, fs), BF16),
            pltpu.VMEM((kv_heads, span, 2 * HEAD), F32),
            pltpu.VMEM((kv_heads, span, 2 * HEAD), BF16),
            pltpu.VMEM((slots, span, 2 * HEAD), BF16),
            pltpu.VMEM((slots, span, 2 * HEAD), BF16),
            pltpu.VMEM((sp // 2, span, 2 * HEAD), BF16),
            pltpu.VMEM((3 * span, 2 * HEAD), BF16),
            pltpu.VMEM((sp, rows, q_cols), BF16),
            pltpu.VMEM((sp, rows, q_cols), BF16),
            pltpu.VMEM((span, HEAD), F32),
            pltpu.VMEM((span, HEAD), F32),
            pltpu.VMEM((rows, window), F32),
            dma((4,)),
            dma((sp,)),
            dma((sp,)),
            dma((sp,)),
            dma((sp,)),
            dma((sp,)),
            dma((sp,)),
            dma((slots,)),
            dma((slots, sp)),
            dma((sp // 2,)),
            dma((sp // 2, sp)),
            dma((2,)),
            dma((2, sp)),
            dma((sp,)),
            dma((sp,)),
        ],
        compiler_params=pltpu.CompilerParams(
            collective_id=0, has_side_effects=True, vmem_limit_bytes=60 * 1024 * 1024
        ),
        name="masked_attention",
    )(*operands)


def solution(mesh):
    in_specs = (
        P(("grp", "blk"), "sp", None),
        P(("grp", "blk"), "sp", "rep"),
        P(),
        P("sp", "rep"),
        P("sp", "rep"),
        P("rep"),
        P("rep"),
        P("grp"),
    )
    out_specs = P(("grp", "blk"), "sp", "rep")
    return jax.shard_map(
        on_device, mesh=mesh, in_specs=in_specs, out_specs=out_specs, check_vma=False
    )
```

```python
import functools
import math

import jax
import jax.numpy as jnp
from jax import lax
from jax.experimental import pallas as pl
from jax.experimental.pallas import tpu as pltpu
from jax.sharding import PartitionSpec as P

HEAD = 128
EPS_VALUE = 1e-06
THETA_BASE = 1000000.0
NEG_FILL = -1e30
MESH = pl.DeviceIdType.MESH
F32, BF16 = jnp.float32, jnp.bfloat16


def kernel(
    sizes,
    hidden_ref,
    queries_ref,
    gain_ref,
    kw_ref,
    vw_ref,
    kb_ref,
    vb_ref,
    docs_ref,
    out_ref,
    hid,
    wts,
    normed,
    feats,
    part_own,
    part_out,
    pair_in,
    pair_out,
    part_in,
    kv,
    qbuf,
    obuf,
    cos_buf,
    sin_buf,
    mask_buf,
    load_sem,
    feat_send,
    feat_recv,
    fwd_send,
    fwd_recv,
    q_send,
    q_recv,
    pair_send,
    pair_recv,
    part_send,
    part_recv,
    kv_send,
    kv_recv,
    o_send,
    o_recv,
):
    sp, blks, reps, rows = sizes
    me = lax.axis_index("sp")
    blk = lax.axis_index("blk")
    rep = lax.axis_index("rep")
    half = rows // reps
    span = sp * rows
    fs = kw_ref.shape[0]
    kv_heads = kw_ref.shape[1] // HEAD
    fold = sp // kv_heads
    my_head = me // fold
    q_cols = queries_ref.shape[2] // sp
    heads = q_cols // HEAD
    window = 2 * span + rows
    docs = docs_ref.shape[0]

    pairs = sp // 2
    my_pair = me // 2
    parity = lax.rem(me, 2)
    slots = pair_in.shape[0]

    def place(k):
        pair = lax.rem(my_pair + k // 2, pairs)
        return 2 * pair + lax.rem(parity + lax.rem(k, 2), 2)

    peer = place
    partner = place(1)

    def slot_head(slot, side):
        return slot if fold > 1 else 2 * slot + side

    barrier = pltpu.get_barrier_semaphore()
    for k in range(1, sp):
        pl.semaphore_signal(barrier, inc=1, device_id={"sp": peer(k)}, device_id_type=MESH)
    for k in range(1, reps):
        pl.semaphore_signal(
            barrier, inc=1, device_id={"rep": lax.rem(rep + k, reps)}, device_id_type=MESH
        )
    for dist in (1, 2):
        pl.semaphore_signal(
            barrier, inc=1, device_id={"blk": lax.rem(blk + dist, blks)}, device_id_type=MESH
        )
        pl.semaphore_signal(
            barrier, inc=1, device_id={"blk": lax.rem(blk + blks - dist, blks)}, device_id_type=MESH
        )

    load_hid = pltpu.make_async_copy(
        hidden_ref.at[0, pl.ds(pl.multiple_of(rep * half, half), half)], hid, load_sem.at[0]
    )
    load_k = pltpu.make_async_copy(kw_ref, wts.at[:, : kv_heads * HEAD], load_sem.at[1])
    load_v = pltpu.make_async_copy(vw_ref, wts.at[:, kv_heads * HEAD :], load_sem.at[2])
    load_q = pltpu.make_async_copy(
        queries_ref.at[0, :, pl.ds(pl.multiple_of(me * q_cols, q_cols), q_cols)],
        qbuf.at[me],
        load_sem.at[3],
    )
    load_hid.start()
    load_k.start()
    load_v.start()
    load_q.start()

    load_hid.wait()
    values = hid[...].astype(F32)
    scale = lax.rsqrt(jnp.mean(values * values, axis=1, keepdims=True) + EPS_VALUE)
    for d in range(sp):
        cols = slice(d * fs, (d + 1) * fs)
        normed[d] = (hid[:, cols].astype(F32) * scale * gain_ref[:, cols]).astype(BF16)

    pl.semaphore_wait(barrier, sp - 1 + reps - 1 + 4)

    def feat_copy(k):
        d = peer(k)
        return pltpu.make_async_remote_copy(
            src_ref=normed.at[d],
            dst_ref=feats.at[me, rep],
            send_sem=feat_send.at[d],
            recv_sem=feat_recv.at[me],
            device_id={"sp": d},
            device_id_type=MESH,
        )

    def feat_arrival(s):
        return pltpu.make_async_remote_copy(
            src_ref=normed.at[0],
            dst_ref=feats.at[s, rep],
            send_sem=feat_send.at[0],
            recv_sem=feat_recv.at[s],
            device_id={"sp": s},
            device_id_type=MESH,
        )

    other = lax.rem(rep + 1, reps)

    def fwd_copy(s, source):
        return pltpu.make_async_remote_copy(
            src_ref=source,
            dst_ref=feats.at[s, rep],
            send_sem=fwd_send.at[s],
            recv_sem=fwd_recv.at[s],
            device_id={"rep": other},
            device_id_type=MESH,
        )

    def fwd_arrival(s):
        return pltpu.make_async_remote_copy(
            src_ref=normed.at[0],
            dst_ref=feats.at[s, other],
            send_sem=fwd_send.at[s],
            recv_sem=fwd_recv.at[s],
            device_id={"rep": other},
            device_id_type=MESH,
        )

    order = list(range(1, sp))
    for k in order:
        feat_copy(k).start()
    fwd_copy(me, normed.at[me]).start()
    feats[me, rep] = normed[me]

    token_base = blk * span
    lanes = lax.broadcasted_iota(jnp.int32, (1, HEAD), 1)
    index = lax.rem(lanes, HEAD // 2).astype(F32)
    inverse = jnp.exp(index * (-2.0 * math.log(THETA_BASE) / HEAD))
    sign = jnp.where(lanes < HEAD // 2, -1.0, 1.0)

    def angle_step(j, carry):
        at = pl.ds(pl.multiple_of(j * rows, rows), rows)
        places = token_base + j * rows + lax.broadcasted_iota(jnp.int32, (rows, HEAD), 0)
        angles = places.astype(F32) * inverse
        cos_buf[at, :] = jnp.cos(angles)
        sin_buf[at, :] = jnp.sin(angles) * sign
        return carry

    lax.fori_loop(0, sp, angle_step, 0)
    load_k.wait()
    load_v.wait()

    def rows_of(j):
        return pl.ds(pl.multiple_of(j * rows, rows), rows)

    def pair_copy(slot, j):
        return pltpu.make_async_remote_copy(
            src_ref=part_out.at[slot_head(slot, 1 - parity), rows_of(j)],
            dst_ref=pair_in.at[slot, rows_of(j)],
            send_sem=pair_send.at[slot],
            recv_sem=pair_recv.at[slot, j],
            device_id={"sp": partner},
            device_id_type=MESH,
        )

    def part_copy(d, j):
        slot = d // fold if fold > 1 else d // 2
        return pltpu.make_async_remote_copy(
            src_ref=pair_out.at[slot, rows_of(j)],
            dst_ref=part_in.at[my_pair, rows_of(j)],
            send_sem=part_send.at[d // 2],
            recv_sem=part_recv.at[my_pair, j],
            device_id={"sp": d},
            device_id_type=MESH,
        )

    def far(k):
        return 2 * lax.rem(my_pair + k, pairs) + parity

    def project(j):
        at = rows_of(j)
        block = feats[j].reshape(rows, fs)
        partial = jnp.dot(block, wts[...], preferred_element_type=F32)
        for h in range(kv_heads):
            key_part = partial[:, h * HEAD : (h + 1) * HEAD]
            value_part = partial[:, (kv_heads + h) * HEAD : (kv_heads + h + 1) * HEAD]
            part_own[h, at, :HEAD] = key_part
            part_own[h, at, HEAD:] = value_part
            part_out[h, at, :HEAD] = key_part.astype(BF16)
            part_out[h, at, HEAD:] = value_part.astype(BF16)
        for slot in range(slots):
            pair_copy(slot, j).start()

    def cross(j):
        at = rows_of(j)
        for slot in range(slots):
            pair_copy(slot, j).wait_recv()
            both = part_own[slot_head(slot, parity), at, :] + pair_in[slot, at, :].astype(F32)
            part_own[slot_head(slot, parity), at, :] = both
            pair_out[slot, at, :] = both.astype(BF16)
        for k in range(1, pairs):
            part_copy(far(k), j).start()

    fwd_arrival(me).wait_recv()
    project(me)

    def arrive(k, carry):
        s = place(k)
        feat_arrival(s).wait_recv()
        fwd_copy(s, feats.at[s, rep]).start()
        fwd_arrival(s).wait_recv()
        project(s)
        cross(place(k - 1))
        return carry

    lax.fori_loop(1, sp, arrive, 0)
    cross(place(sp - 1))

    def q_copy(d):
        return pltpu.make_async_remote_copy(
            src_ref=queries_ref.at[0, :, pl.ds(pl.multiple_of(d * q_cols, q_cols), q_cols)],
            dst_ref=qbuf.at[me],
            send_sem=q_send.at[d],
            recv_sem=q_recv.at[me],
            device_id={"sp": d},
            device_id_type=MESH,
        )

    def q_arrival(s):
        return pltpu.make_async_remote_copy(
            src_ref=qbuf.at[s],
            dst_ref=qbuf.at[s],
            send_sem=q_send.at[s],
            recv_sem=q_recv.at[s],
            device_id={"sp": s},
            device_id_type=MESH,
        )

    for k in reversed(order):
        q_copy(peer(k)).start()

    for piece in (0, 1):

        @pl.when(blk < 2 - piece)
        def _():
            kv[pl.ds(piece * span, span), :] = jnp.zeros((span, 2 * HEAD), BF16)


    def own_shift(ref):
        row = ref[...].astype(F32).reshape(1, kv_heads * HEAD)
        mine = row[:, :HEAD]
        for h in range(1, kv_heads):
            mine = jnp.where(my_head == h, row[:, h * HEAD : (h + 1) * HEAD], mine)
        return mine

    key_shift = own_shift(kb_ref)
    value_shift = own_shift(vb_ref)

    relay = blks == 4

    def kv_copy(piece, dist, j):
        return pltpu.make_async_remote_copy(
            src_ref=kv.at[pl.ds(pl.multiple_of(piece * span + j * rows, rows), rows)],
            dst_ref=kv.at[pl.ds(pl.multiple_of((2 - dist) * span + j * rows, rows), rows)],
            send_sem=kv_send.at[dist - 1],
            recv_sem=kv_recv.at[dist - 1, j],
            device_id={"blk": lax.rem(blk + dist, blks)},
            device_id_type=MESH,
        )

    def kv_pass(j):
        kv_copy(2, 2, j).wait_recv()
        pltpu.make_async_remote_copy(
            src_ref=kv.at[pl.ds(pl.multiple_of(j * rows, rows), rows)],
            dst_ref=kv.at[pl.ds(pl.multiple_of(span + j * rows, rows), rows)],
            send_sem=kv_send.at[0],
            recv_sem=kv_recv.at[0, j],
            device_id={"blk": lax.rem(blk + blks - 1, blks)},
            device_id_type=MESH,
        ).start()

    near = blk + 1 < blks
    if relay:
        near = near & (blk != 1)
    sends = {1: near, 2: blk + 2 < blks}

    def finish(i, carry):
        j = place(i)
        at = rows_of(j)
        total = part_own[my_head, at, :]
        for k in range(1, pairs):
            s = lax.rem(my_pair + k, pairs)
            pltpu.make_async_remote_copy(
                src_ref=part_in.at[s, at],
                dst_ref=part_in.at[s, at],
                send_sem=part_send.at[s],
                recv_sem=part_recv.at[s, j],
                device_id={"sp": far(k)},
                device_id_type=MESH,
            ).wait_recv()
            total = total + part_in[s, at, :].astype(F32)
        keys = total[:, :HEAD] + key_shift
        turned = keys * cos_buf[at, :] + pltpu.roll(keys, HEAD // 2, 1) * sin_buf[at, :]
        put = pl.ds(pl.multiple_of(2 * span + j * rows, rows), rows)
        kv[put, :HEAD] = turned.astype(BF16)
        kv[put, HEAD:] = (total[:, HEAD:] + value_shift).astype(BF16)
        for dist in (2, 1):

            @pl.when(sends[dist])
            def _():
                kv_copy(2, dist, j).start()

        if relay:

            @pl.when((blk == 3) & (i >= 1))
            def _():
                kv_pass(place(i - 1))

        return carry

    lax.fori_loop(0, sp, finish, 0)
    if relay:

        @pl.when(blk == 3)
        def _():
            kv_pass(place(sp - 1))


    ends = []
    running = jnp.int32(0)
    for d in range(docs):
        running = running + docs_ref[d]
        ends.append(running)

    load_q.wait()
    for dist in (1, 2):

        arrives = blk >= dist
        if relay and dist == 2:
            arrives = arrives & (blk != 3)

        @pl.when(arrives)
        def _():
            for j in range(sp):
                kv_copy(2, dist, j).wait_recv()

    exponent = math.log2(math.e) / math.sqrt(HEAD)

    def attend(t):
        query_at = token_base + t * rows + lax.broadcasted_iota(jnp.int32, (rows, HEAD), 0)
        first = jnp.zeros((rows, HEAD), jnp.int32)
        for end in ends:
            first = jnp.where(query_at >= end, end, first)
        key_base = token_base - 2 * span + t * rows
        for c in range(window // HEAD):
            key_at = key_base + c * HEAD + lax.broadcasted_iota(jnp.int32, (rows, HEAD), 1)
            seen = (key_at >= first) & (key_at <= query_at)
            mask_buf[:, c * HEAD : (c + 1) * HEAD] = jnp.where(seen, 0.0, NEG_FILL)
        at = pl.ds(pl.multiple_of(t * rows, rows), window)
        for h in range(heads):
            cols = slice(h * HEAD, (h + 1) * HEAD)
            scores = lax.dot_general(
                qbuf[t, :, cols], kv[at, :HEAD], (((1,), (1,)), ((), ())), preferred_element_type=F32
            )
            scores = scores + mask_buf[...]
            largest = jnp.max(scores, axis=1, keepdims=True)
            weights = jnp.exp2((scores - largest) * exponent).astype(BF16)
            total = jnp.sum(weights.astype(F32), axis=1, keepdims=True)
            summed = jnp.dot(weights, kv[at, HEAD:], preferred_element_type=F32)
            obuf[t, :, cols] = (summed / total).astype(BF16)

    my_cols = pl.ds(pl.multiple_of(me * q_cols, q_cols), q_cols)

    def o_copy(d):
        return pltpu.make_async_remote_copy(
            src_ref=obuf.at[d],
            dst_ref=out_ref.at[0, :, my_cols],
            send_sem=o_send.at[d],
            recv_sem=o_recv.at[me],
            device_id={"sp": d},
            device_id_type=MESH,
        )

    def o_arrival(s):
        return pltpu.make_async_remote_copy(
            src_ref=obuf.at[s],
            dst_ref=out_ref.at[0, :, pl.ds(pl.multiple_of(s * q_cols, q_cols), q_cols)],
            send_sem=o_send.at[s],
            recv_sem=o_recv.at[s],
            device_id={"sp": s},
            device_id_type=MESH,
        )

    def each(k, carry):
        t = place(sp - k)
        q_arrival(t).wait_recv()
        attend(t)
        o_copy(t).start()
        return carry

    lax.fori_loop(1, sp, each, 0)
    attend(me)
    out_ref[0, :, my_cols] = obuf[me]

    for k in order:
        d = peer(k)
        o_arrival(d).wait_recv()
        o_copy(d).wait_send()
        feat_copy(k).wait_send()
        q_copy(d).wait_send()
        fwd_copy(d, feats.at[d, rep]).wait_send()
    fwd_copy(me, normed.at[me]).wait_send()

    def sent(sem, source):
        pltpu.make_async_remote_copy(
            src_ref=source,
            dst_ref=source,
            send_sem=sem,
            recv_sem=part_recv.at[0, 0],
            device_id={"sp": partner},
            device_id_type=MESH,
        ).wait_send()

    for slot in range(slots):
        sent(pair_send.at[slot], pair_in.at[slot])
    for k in range(1, pairs):
        sent(part_send.at[far(k) // 2], part_in.at[0])
    for dist in (1, 2):

        shipped = sends[dist]
        if relay and dist == 1:
            shipped = shipped | (blk == 3)

        @pl.when(shipped)
        def _():
            sent(kv_send.at[dist - 1], kv.at[pl.ds(0, span)])


def heads_kernel(
    sizes,
    hidden_ref,
    queries_ref,
    gain_ref,
    kw_ref,
    vw_ref,
    kb_ref,
    vb_ref,
    docs_ref,
    out_ref,
    hid,
    wts,
    normed,
    feats,
    own,
    up_in,
    up_out,
    down_in,
    down_out,
    self_out,
    self_in,
    up_last,
    down_last,
    kv,
    qbuf,
    obuf,
    total,
    cos_buf,
    sin_buf,
    mask_buf,
    load_sem,
    feat_send,
    feat_recv,
    fwd_send,
    fwd_recv,
    q_send,
    q_recv,
    self_send,
    self_recv,
    up_send,
    up_recv,
    up_last_send,
    up_last_recv,
    down_send,
    down_recv,
    down_last_send,
    down_last_recv,
    rise_send,
    rise_recv,
    fall_send,
    fall_recv,
    o_send,
    o_recv,
):
    sp, blks, reps, rows, chunks = sizes
    me = lax.axis_index("sp")
    blk = lax.axis_index("blk")
    rep = lax.axis_index("rep")
    span = sp * rows
    cut = rows // chunks
    part = cut // reps
    fs = kw_ref.shape[0]
    q_cols = queries_ref.shape[2] // blks
    heads = q_cols // HEAD
    docs = docs_ref.shape[0]
    window = 2 * span + rows
    last = sp - 1
    pair = 2 * HEAD

    turn = 2 * lax.rem(blk, 2) - 1

    def group(k):
        return lax.rem(blk + blks + k * turn, blks)

    barrier = pltpu.get_barrier_semaphore()
    for k in range(1, sp):
        pl.semaphore_signal(
            barrier, inc=1, device_id={"sp": lax.rem(me + k, sp)}, device_id_type=MESH
        )
    for k in range(1, reps):
        pl.semaphore_signal(
            barrier, inc=1, device_id={"rep": lax.rem(rep + k, reps)}, device_id_type=MESH
        )
    for k in range(1, blks):
        pl.semaphore_signal(barrier, inc=1, device_id={"blk": group(k)}, device_id_type=MESH)

        @pl.when(me > 0)
        def _():
            pl.semaphore_signal(
                barrier, inc=1, device_id={"sp": me - 1, "blk": group(k)}, device_id_type=MESH
            )

        @pl.when(me < last)
        def _():
            pl.semaphore_signal(
                barrier, inc=1, device_id={"sp": me + 1, "blk": group(k)}, device_id_type=MESH
            )

    def load_hid(q):
        return pltpu.make_async_copy(
            hidden_ref.at[0, pl.ds(pl.multiple_of(q * cut + rep * part, part), part)],
            hid.at[q],
            load_sem.at[q],
        )

    def load_w(g, side):
        source = vw_ref if side else kw_ref
        return pltpu.make_async_copy(
            source.at[:, g * HEAD : (g + 1) * HEAD],
            wts.at[:, (2 * g + side) * HEAD : (2 * g + side + 1) * HEAD],
            load_sem.at[chunks + 2 * g + side],
        )

    own_cols = pl.ds(pl.multiple_of(blk * q_cols, q_cols), q_cols)
    load_q = pltpu.make_async_copy(
        queries_ref.at[0, :, own_cols], qbuf.at[blk], load_sem.at[chunks + 2 * blks]
    )
    for q in range(chunks):
        load_hid(q).start()
    for g in range(blks):
        load_w(g, 0).start()
        load_w(g, 1).start()
    load_q.start()

    def feat_copy(q, d):
        return pltpu.make_async_remote_copy(
            src_ref=normed.at[q, d],
            dst_ref=feats.at[q, me, rep],
            send_sem=feat_send,
            recv_sem=feat_recv.at[q, me],
            device_id={"sp": d},
            device_id_type=MESH,
        )

    def feat_arrival(q, s):
        return pltpu.make_async_remote_copy(
            src_ref=normed.at[q, 0],
            dst_ref=feats.at[q, s, rep],
            send_sem=feat_send,
            recv_sem=feat_recv.at[q, s],
            device_id={"sp": s},
            device_id_type=MESH,
        )

    other = lax.rem(rep + 1, reps)

    def fwd_copy(q, s, source):
        return pltpu.make_async_remote_copy(
            src_ref=source,
            dst_ref=feats.at[q, s, rep],
            send_sem=fwd_send,
            recv_sem=fwd_recv.at[q],
            device_id={"rep": other},
            device_id_type=MESH,
        )

    def q_copy(g):
        return pltpu.make_async_remote_copy(
            src_ref=queries_ref.at[0, :, pl.ds(pl.multiple_of(g * q_cols, q_cols), q_cols)],
            dst_ref=qbuf.at[blk],
            send_sem=q_send,
            recv_sem=q_recv,
            device_id={"blk": g},
            device_id_type=MESH,
        )

    def norm(q):
        load_hid(q).wait()
        values = hid[q].astype(F32)
        scale = lax.rsqrt(jnp.mean(values * values, axis=1, keepdims=True) + EPS_VALUE)
        for d in range(sp):
            cols = slice(d * fs, (d + 1) * fs)
            normed[q, d] = (hid[q, :, cols].astype(F32) * scale * gain_ref[:, cols]).astype(BF16)

    norm(0)
    peers = sp - 1 + reps - 1 + blks - 1

    @pl.when((me == 0) | (me == last))
    def _():
        pl.semaphore_wait(barrier, peers + blks - 1)

    @pl.when((me > 0) & (me < last))
    def _():
        pl.semaphore_wait(barrier, peers + 2 * (blks - 1))

    for q in range(chunks):
        if q > 0:
            norm(q)
        for step in range(1, sp):
            far = jnp.where(rep == 0, step, sp - step)

            @pl.when(me + far < sp)
            def _():
                feat_copy(q, me + far).start()

            @pl.when(me >= far)
            def _():
                feat_copy(q, me - far).start()

        fwd_copy(q, me, normed.at[q, me]).start()
        feats[q, me, rep] = normed[q, me]
    for k in range(1, blks):
        q_copy(group(k)).start()

    lanes = lax.broadcasted_iota(jnp.int32, (1, HEAD), 1)
    index = lax.rem(lanes, HEAD // 2).astype(F32)
    inverse = jnp.exp(index * (-2.0 * math.log(THETA_BASE) / HEAD))
    sign = jnp.where(lanes < HEAD // 2, -1.0, 1.0)

    def angle_step(c, carry):
        places = c * span + me * rows + lax.broadcasted_iota(jnp.int32, (rows, HEAD), 0)
        angles = places.astype(F32) * inverse
        cos_buf[c] = jnp.cos(angles)
        sin_buf[c] = jnp.sin(angles) * sign
        return carry

    lax.fori_loop(0, blks, angle_step, 0)
    kv[: 2 * span, :pair] = jnp.zeros((2 * span, pair), BF16)
    kv[:, pair:] = jnp.ones((kv.shape[0], HEAD), BF16)

    def own_shift(ref):
        row = ref[...].astype(F32).reshape(1, blks * HEAD)
        mine = row[:, :HEAD]
        for g in range(1, blks):
            mine = jnp.where(blk == g, row[:, g * HEAD : (g + 1) * HEAD], mine)
        return mine

    key_shift = own_shift(kb_ref)
    value_shift = own_shift(vb_ref)

    def landed(sem, ref):
        pltpu.make_async_remote_copy(
            src_ref=ref,
            dst_ref=ref,
            send_sem=sem,
            recv_sem=sem,
            device_id={"rep": other},
            device_id_type=MESH,
        ).wait_recv()

    def left(sem, ref):
        pltpu.make_async_remote_copy(
            src_ref=ref,
            dst_ref=ref,
            send_sem=sem,
            recv_sem=sem,
            device_id={"rep": other},
            device_id_type=MESH,
        ).wait_send()

    def self_copy(q, g):
        return pltpu.make_async_remote_copy(
            src_ref=self_out.at[q, g],
            dst_ref=self_in.at[q, blk],
            send_sem=self_send,
            recv_sem=self_recv.at[q],
            device_id={"blk": g},
            device_id_type=MESH,
        )

    def project(q):
        for far in range(1, sp):

            @pl.when(me >= far)
            def _():
                feat_arrival(q, me - far).wait_recv()
                fwd_copy(q, me - far, feats.at[q, me - far, rep]).start()

            @pl.when(me + far < sp)
            def _():
                feat_arrival(q, me + far).wait_recv()
                fwd_copy(q, me + far, feats.at[q, me + far, rep]).start()

        landed(fwd_recv.at[q], normed.at[q])
        partial = jnp.dot(
            feats[q].reshape(sp * cut, fs), wts[...], preferred_element_type=F32
        )
        for j in range(sp):
            for g in range(blks):
                own[q, j, g] = partial[j * cut : (j + 1) * cut, g * pair : (g + 1) * pair]

    def keep(q):
        for k in range(1, blks):
            g = group(k)
            self_out[q, g] = own[q, me, g].astype(BF16)
            self_copy(q, g).start()
        self_in[q, blk] = own[q, me, blk].astype(BF16)

    def hop(q, t, d, up):
        to = t + 1 if up else t - 1
        came = t > 0 if up else t < last
        inbound, outbound = (up_in, up_out) if up else (down_in, down_out)
        sent, arrived = (up_send, up_recv) if up else (down_send, down_recv)
        lands = up_last if up else down_last
        land_sent, landed_sem = (up_last_send, up_last_recv) if up else (down_last_send, down_last_recv)
        if came:
            landed(arrived.at[q, d], inbound.at[q, d])
        for g in range(blks):
            value = own[q, d, g]
            if came:
                value = value + inbound[q, d, g].astype(F32)
            outbound[q, d, g] = value.astype(BF16)
        if d != to:
            pltpu.make_async_remote_copy(
                src_ref=outbound.at[q, d],
                dst_ref=inbound.at[q, d],
                send_sem=sent,
                recv_sem=arrived.at[q, d],
                device_id={"sp": to},
                device_id_type=MESH,
            ).start()
        else:
            for k in range(blks):
                g = group(k)
                pltpu.make_async_remote_copy(
                    src_ref=outbound.at[q, d, g],
                    dst_ref=lands.at[q, blk],
                    send_sem=land_sent,
                    recv_sem=landed_sem.at[q],
                    device_id={"sp": to, "blk": g},
                    device_id_type=MESH,
                ).start()

    def relay(q, t, d):
        @pl.when(me == t)
        def _():
            hop(q, t, d, True)

        @pl.when(me == last - t)
        def _():
            hop(q, last - t, last - d, False)

    def place(q, c, j):
        return pl.ds(pl.multiple_of(2 * span + (c * sp + j) * rows + q * cut, cut), cut)

    sent_cols = slice(0, pair)

    def rise(q, j):
        for c in range(blks):
            pltpu.make_async_remote_copy(
                src_ref=kv.at[place(q, c, j), sent_cols],
                dst_ref=kv.at[place(q, c, j), sent_cols],
                send_sem=rise_send,
                recv_sem=rise_recv.at[q, j],
                device_id={"sp": me + 1},
                device_id_type=MESH,
            ).start()

    def fall(q, j):
        for c in range(blks - 1):
            pltpu.make_async_remote_copy(
                src_ref=kv.at[place(q, c, j), sent_cols],
                dst_ref=kv.at[place(q, c, j), sent_cols],
                send_sem=fall_send,
                recv_sem=fall_recv.at[q, j],
                device_id={"sp": me - 1},
                device_id_type=MESH,
            ).start()

    def close(q):
        landed(self_recv.at[q], self_in.at[q, pl.ds(0, blks - 1)])
        total[...] = self_in[q].astype(F32)

        @pl.when(me > 0)
        def _():
            landed(up_last_recv.at[q], up_last.at[q])
            total[...] = total[...] + up_last[q].astype(F32)

        @pl.when(me < last)
        def _():
            landed(down_last_recv.at[q], down_last.at[q])
            total[...] = total[...] + down_last[q].astype(F32)

        at = slice(q * cut, (q + 1) * cut)
        for c in range(blks):
            keys = total[c, :, :HEAD] + key_shift
            turned = keys * cos_buf[c, at] + pltpu.roll(keys, HEAD // 2, 1) * sin_buf[c, at]
            kv[place(q, c, me), :HEAD] = turned.astype(BF16)
            kv[place(q, c, me), HEAD:pair] = (total[c, :, HEAD:] + value_shift).astype(BF16)

        @pl.when(me < last)
        def _():
            rise(q, me)

        @pl.when(me > 0)
        def _():
            fall(q, me)

    def close_inner(q):
        @pl.when((me > 0) & (me < last))
        def _():
            close(q)

    def close_outer(q):
        @pl.when((me == 0) | (me == last))
        def _():
            close(q)

    every = kv.at[pl.ds(0, blks * cut), sent_cols]
    fallen = kv.at[pl.ds(0, (blks - 1) * cut), sent_cols]

    def gather(q, t, j):
        @pl.when(me == t)
        def _():
            landed(rise_recv.at[q, j], every)
            if t < last:
                rise(q, j)

        @pl.when(me == last - t)
        def _():
            landed(fall_recv.at[q, last - j], fallen)
            if t < last:
                fall(q, last - j)

    ends = []
    running = jnp.int32(0)
    for d in range(docs):
        running = running + docs_ref[d]
        ends.append(running)

    exponent = math.log2(math.e) / math.sqrt(HEAD)

    def mask_step(c, carry):
        query_at = c * span + me * rows + lax.broadcasted_iota(jnp.int32, (rows, HEAD), 0)
        first = jnp.zeros((rows, HEAD), jnp.int32)
        for end in ends:
            first = jnp.where(query_at >= end, end, first)
        base = c * span + me * rows - 2 * span
        for piece in range(window // HEAD):
            key_at = base + piece * HEAD + lax.broadcasted_iota(jnp.int32, (rows, HEAD), 1)
            seen = (key_at >= first) & (key_at <= query_at)
            mask_buf[c, :, piece * HEAD : (piece + 1) * HEAD] = jnp.where(seen, 0.0, NEG_FILL)
        return carry

    def attend(c):
        at = pl.ds(pl.multiple_of(c * span + me * rows, rows), window)
        for h in range(0, heads, 2):
            parts = [slice(n * HEAD, (n + 1) * HEAD) for n in range(h, min(h + 2, heads))]
            stacked = jnp.concatenate([qbuf[c, :, cols] for cols in parts], axis=0)
            scores = lax.dot_general(
                stacked, kv[at, :HEAD], (((1,), (1,)), ((), ())), preferred_element_type=F32
            )
            scores = scores.reshape(len(parts), rows, window) + mask_buf[c][None]
            scores = scores.reshape(len(parts) * rows, window)
            largest = jnp.max(scores, axis=1, keepdims=True)
            weights = jnp.exp2((scores - largest) * exponent).astype(BF16)
            summed = jnp.dot(weights, kv[at, HEAD:], preferred_element_type=F32)
            result = (summed[:, :HEAD] / summed[:, HEAD:]).astype(BF16)
            for n, cols in enumerate(parts):
                obuf[c, :, cols] = result[n * rows : (n + 1) * rows]

    def o_copy(c):
        return pltpu.make_async_remote_copy(
            src_ref=obuf.at[c],
            dst_ref=out_ref.at[0, :, own_cols],
            send_sem=o_send,
            recv_sem=o_recv,
            device_id={"blk": c},
            device_id_type=MESH,
        )

    def weights_in():
        for g in range(blks):
            load_w(g, 0).wait()
            load_w(g, 1).wait()

    def queries_in():
        load_q.wait()
        landed(q_recv, qbuf.at[pl.ds(0, blks - 1)])

    def finish(k, carry):
        attend(group(k))
        o_copy(group(k)).start()
        return carry

    unit, hop_time, lead = 5.6 / chunks, 3.3, 13.0
    inner_late, outer_late, gather_late, first_late = 1.0, 0.0, 1.5, 0.0
    hold = 0
    feed_first, feed_step = 10.0, 11.2 / chunks
    queue = []
    for q in range(chunks + hold):
        if q < chunks:
            queue.append((q, last))
        if q >= hold and hold:
            queue.append((q - hold, 1))
        if q < chunks:
            queue.extend((q, d) for d in range(last - 1, 0 if not hold else 1, -1))
    came = {item: lead + unit * (n + 1) + 1.0 for n, item in enumerate(queue)}
    fed = lead + unit * len(queue) + 1.0
    events = []
    for q in range(chunks):

        def first_step(q=q):
            if q == 0:
                weights_in()
            project(q)
            begin = queue.index((q, last))
            end = queue.index((q + 1, last)) if q + 1 < chunks else len(queue)
            for n in range(begin, end):
                relay(queue[n][0], 0, queue[n][1])
            keep(q)

        events.append((feed_first + feed_step * q, first_step, ()))
        for t in range(1, last):
            for d in range(last, t, -1):
                events.append((came[q, d] + hop_time * (t - 1), relay, (q, t, d)))
        inner = max(came[q, 1], came[q, last - 1] + hop_time) + inner_late
        outer = came[q, last] + hop_time * (last - 1) + outer_late
        events.append((inner, close_inner, (q,)))
        events.append((outer, close_outer, (q,)))
        for j in range(last):
            for t in range(j + 1, sp):
                if j == 0:
                    come = max(outer + hop_time, fed + unit * (q + 1)) + first_late
                else:
                    come = inner + hop_time + gather_late
                when = come + (t - j - 1) * hop_time
                events.append((1000.0 + when if t == last else when, gather, (q, t, j)))

    def masks_outer():
        @pl.when((me == 0) | (me == last))
        def _():
            lax.fori_loop(0, blks, mask_step, 0)

    def masks_inner():
        @pl.when((me > 0) & (me < last))
        def _():
            lax.fori_loop(0, blks, mask_step, 0)

    events.append((feed_first + feed_step * (chunks - 1) + 0.1, masks_outer, ()))
    events.append((999.0, masks_inner, ()))
    events.sort(key=lambda e: e[0])
    for _, step, taken in events:
        step(*taken)
    queries_in()

    lax.fori_loop(1, blks, finish, 0)
    attend(blk)
    out_ref[0, :, own_cols] = obuf[blk]

    some = pl.ds(0, blks - 1)
    left(feat_send, normed.at[:, pl.ds(0, sp - 1)])
    left(fwd_send, normed)
    left(self_send, self_out.at[:, some])
    left(q_send, qbuf.at[some])
    for t in range(sp):

        @pl.when(me == t)
        def _():
            if t < last - 1:
                left(up_send, up_out.at[:, pl.ds(0, last - t - 1)])
            if t > 1:
                left(down_send, down_out.at[:, pl.ds(0, t - 1)])
            if t < last:
                left(up_last_send, up_last)
                left(rise_send, kv.at[pl.ds(0, blks * rows * (t + 1)), sent_cols])
            if t > 0:
                left(down_last_send, down_last)
                left(fall_send, kv.at[pl.ds(0, (blks - 1) * rows * (sp - t)), sent_cols])

    landed(o_recv, obuf.at[some])
    left(o_send, obuf.at[some])


CHUNKS = 4


def heads_call(operands, sp, blks, reps):
    hidden, queries, _, key_matrix = operands[:4]
    rows, width = hidden.shape[1:]
    chunks = CHUNKS
    cut = rows // chunks
    span = rows * sp
    fs, kv_cols = key_matrix.shape
    q_cols = queries.shape[2] // blks
    pair = 2 * HEAD
    vmem = pl.BlockSpec(memory_space=pltpu.VMEM)
    anywhere = pl.BlockSpec(memory_space=pl.ANY)
    smem = pl.BlockSpec(memory_space=pltpu.SMEM)
    dma = pltpu.SemaphoreType.DMA
    by_sp, each = dma((chunks, sp)), dma((chunks,))
    line = pltpu.VMEM((chunks, sp, blks, cut, pair), BF16)
    spot = pltpu.VMEM((chunks, blks, cut, pair), BF16)
    return pl.pallas_call(
        functools.partial(heads_kernel, (sp, blks, reps, rows, chunks)),
        out_shape=pltpu.VMEM(queries.shape, BF16),
        in_specs=[anywhere, anywhere, vmem, anywhere, anywhere, vmem, vmem, smem],
        out_specs=vmem,
        scratch_shapes=[
            pltpu.VMEM((chunks, cut // reps, width), BF16),
            pltpu.VMEM((fs, 2 * kv_cols), BF16),
            pltpu.VMEM((chunks, sp, cut // reps, fs), BF16),
            pltpu.VMEM((chunks, sp, reps, cut // reps, fs), BF16),
            pltpu.VMEM((chunks, sp, blks, cut, pair), F32),
            line,
            line,
            line,
            line,
            spot,
            spot,
            spot,
            spot,
            pltpu.VMEM(((2 + blks) * span, 3 * HEAD), BF16),
            pltpu.VMEM((blks, rows, q_cols), BF16),
            pltpu.VMEM((blks, rows, q_cols), BF16),
            pltpu.VMEM((blks, cut, pair), F32),
            pltpu.VMEM((blks, rows, HEAD), F32),
            pltpu.VMEM((blks, rows, HEAD), F32),
            pltpu.VMEM((blks, rows, 2 * span + rows), F32),
            dma((chunks + 2 * blks + 1,)),
            dma,
            by_sp,
            dma,
            each,
            dma,
            dma,
            dma,
            each,
            dma,
            by_sp,
            dma,
            each,
            dma,
            by_sp,
            dma,
            each,
            dma,
            by_sp,
            dma,
            by_sp,
            dma,
            dma,
        ],
        compiler_params=pltpu.CompilerParams(
            collective_id=0, has_side_effects=True, vmem_limit_bytes=60 * 1024 * 1024
        ),
        name="masked_attention",
    )(*operands)


def on_device(
    hidden,
    queries,
    norm_gain,
    key_matrix,
    value_matrix,
    key_shift_bias,
    value_shift_bias,
    doc_lengths,
):
    sp = lax.axis_size("sp")
    blks = lax.axis_size("blk")
    reps = lax.axis_size("rep")
    rows, width = hidden.shape[1:]
    half = rows // reps
    span = rows * sp
    fs = key_matrix.shape[0]
    kv_cols = key_matrix.shape[1]
    kv_heads = kv_cols // HEAD
    q_cols = queries.shape[2] // sp
    window = 2 * span + rows
    slots = kv_heads if sp > kv_heads else kv_heads // 2
    operands = (
        hidden,
        queries,
        norm_gain.reshape(1, width),
        key_matrix,
        value_matrix,
        key_shift_bias,
        value_shift_bias,
        doc_lengths,
    )
    if blks == kv_heads:
        return heads_call(operands, sp, blks, reps)
    vmem = pl.BlockSpec(memory_space=pltpu.VMEM)
    anywhere = pl.BlockSpec(memory_space=pl.ANY)
    smem = pl.BlockSpec(memory_space=pltpu.SMEM)
    dma = pltpu.SemaphoreType.DMA
    return pl.pallas_call(
        functools.partial(kernel, (sp, blks, reps, rows)),
        out_shape=jax.ShapeDtypeStruct(queries.shape, BF16),
        in_specs=[anywhere, anywhere, vmem, anywhere, anywhere, vmem, vmem, smem],
        out_specs=vmem,
        scratch_shapes=[
            pltpu.VMEM((half, width), BF16),
            pltpu.VMEM((fs, 2 * kv_cols), BF16),
            pltpu.VMEM((sp, half, fs), BF16),
            pltpu.VMEM((sp, reps, half, fs), BF16),
            pltpu.VMEM((kv_heads, span, 2 * HEAD), F32),
            pltpu.VMEM((kv_heads, span, 2 * HEAD), BF16),
            pltpu.VMEM((slots, span, 2 * HEAD), BF16),
            pltpu.VMEM((slots, span, 2 * HEAD), BF16),
            pltpu.VMEM((sp // 2, span, 2 * HEAD), BF16),
            pltpu.VMEM((3 * span, 2 * HEAD), BF16),
            pltpu.VMEM((sp, rows, q_cols), BF16),
            pltpu.VMEM((sp, rows, q_cols), BF16),
            pltpu.VMEM((span, HEAD), F32),
            pltpu.VMEM((span, HEAD), F32),
            pltpu.VMEM((rows, window), F32),
            dma((4,)),
            dma((sp,)),
            dma((sp,)),
            dma((sp,)),
            dma((sp,)),
            dma((sp,)),
            dma((sp,)),
            dma((slots,)),
            dma((slots, sp)),
            dma((sp // 2,)),
            dma((sp // 2, sp)),
            dma((2,)),
            dma((2, sp)),
            dma((sp,)),
            dma((sp,)),
        ],
        compiler_params=pltpu.CompilerParams(
            collective_id=0, has_side_effects=True, vmem_limit_bytes=60 * 1024 * 1024
        ),
        name="masked_attention",
    )(*operands)


def solution(mesh):
    in_specs = (
        P(("grp", "blk"), "sp", None),
        P(("grp", "blk"), "sp", "rep"),
        P(),
        P("sp", "rep"),
        P("sp", "rep"),
        P("rep"),
        P("rep"),
        P("grp"),
    )
    out_specs = P(("grp", "blk"), "sp", "rep")
    return jax.shard_map(
        on_device, mesh=mesh, in_specs=in_specs, out_specs=out_specs, check_vma=False
    )
```

```python
import functools
import math

import jax
import jax.numpy as jnp
from jax import lax
from jax.experimental import pallas as pl
from jax.experimental.pallas import tpu as pltpu
from jax.sharding import PartitionSpec as P

HEAD = 128
EPS_VALUE = 1e-06
THETA_BASE = 1000000.0
NEG_FILL = -1e30
MESH = pl.DeviceIdType.MESH
F32, BF16 = jnp.float32, jnp.bfloat16


def kernel(
    sizes,
    hidden_ref,
    queries_ref,
    gain_ref,
    kw_ref,
    vw_ref,
    kb_ref,
    vb_ref,
    docs_ref,
    out_ref,
    hid,
    wts,
    normed,
    feats,
    part_own,
    part_out,
    pair_in,
    pair_out,
    part_in,
    kv,
    qbuf,
    obuf,
    cos_buf,
    sin_buf,
    mask_buf,
    load_sem,
    feat_send,
    feat_recv,
    fwd_send,
    fwd_recv,
    q_send,
    q_recv,
    pair_send,
    pair_recv,
    part_send,
    part_recv,
    kv_send,
    kv_recv,
    o_send,
    o_recv,
):
    sp, blks, reps, rows = sizes
    me = lax.axis_index("sp")
    blk = lax.axis_index("blk")
    rep = lax.axis_index("rep")
    half = rows // reps
    span = sp * rows
    fs = kw_ref.shape[0]
    kv_heads = kw_ref.shape[1] // HEAD
    fold = sp // kv_heads
    my_head = me // fold
    q_cols = queries_ref.shape[2] // sp
    heads = q_cols // HEAD
    window = 2 * span + rows
    docs = docs_ref.shape[0]

    pairs = sp // 2
    my_pair = me // 2
    parity = lax.rem(me, 2)
    slots = pair_in.shape[0]

    def place(k):
        pair = lax.rem(my_pair + k // 2, pairs)
        return 2 * pair + lax.rem(parity + lax.rem(k, 2), 2)

    peer = place
    partner = place(1)

    def slot_head(slot, side):
        return slot if fold > 1 else 2 * slot + side

    barrier = pltpu.get_barrier_semaphore()
    for k in range(1, sp):
        pl.semaphore_signal(barrier, inc=1, device_id={"sp": peer(k)}, device_id_type=MESH)
    for k in range(1, reps):
        pl.semaphore_signal(
            barrier, inc=1, device_id={"rep": lax.rem(rep + k, reps)}, device_id_type=MESH
        )
    for dist in (1, 2):
        pl.semaphore_signal(
            barrier, inc=1, device_id={"blk": lax.rem(blk + dist, blks)}, device_id_type=MESH
        )
        pl.semaphore_signal(
            barrier, inc=1, device_id={"blk": lax.rem(blk + blks - dist, blks)}, device_id_type=MESH
        )

    load_hid = pltpu.make_async_copy(
        hidden_ref.at[0, pl.ds(pl.multiple_of(rep * half, half), half)], hid, load_sem.at[0]
    )
    load_k = pltpu.make_async_copy(kw_ref, wts.at[:, : kv_heads * HEAD], load_sem.at[1])
    load_v = pltpu.make_async_copy(vw_ref, wts.at[:, kv_heads * HEAD :], load_sem.at[2])
    load_q = pltpu.make_async_copy(
        queries_ref.at[0, :, pl.ds(pl.multiple_of(me * q_cols, q_cols), q_cols)],
        qbuf.at[me],
        load_sem.at[3],
    )
    load_hid.start()
    load_k.start()
    load_v.start()
    load_q.start()

    load_hid.wait()
    values = hid[...].astype(F32)
    scale = lax.rsqrt(jnp.mean(values * values, axis=1, keepdims=True) + EPS_VALUE)
    for d in range(sp):
        cols = slice(d * fs, (d + 1) * fs)
        normed[d] = (hid[:, cols].astype(F32) * scale * gain_ref[:, cols]).astype(BF16)

    pl.semaphore_wait(barrier, sp - 1 + reps - 1 + 4)

    def feat_copy(k):
        d = peer(k)
        return pltpu.make_async_remote_copy(
            src_ref=normed.at[d],
            dst_ref=feats.at[me, rep],
            send_sem=feat_send.at[d],
            recv_sem=feat_recv.at[me],
            device_id={"sp": d},
            device_id_type=MESH,
        )

    def feat_arrival(s):
        return pltpu.make_async_remote_copy(
            src_ref=normed.at[0],
            dst_ref=feats.at[s, rep],
            send_sem=feat_send.at[0],
            recv_sem=feat_recv.at[s],
            device_id={"sp": s},
            device_id_type=MESH,
        )

    other = lax.rem(rep + 1, reps)

    def fwd_copy(s, source):
        return pltpu.make_async_remote_copy(
            src_ref=source,
            dst_ref=feats.at[s, rep],
            send_sem=fwd_send.at[s],
            recv_sem=fwd_recv.at[s],
            device_id={"rep": other},
            device_id_type=MESH,
        )

    def fwd_arrival(s):
        return pltpu.make_async_remote_copy(
            src_ref=normed.at[0],
            dst_ref=feats.at[s, other],
            send_sem=fwd_send.at[s],
            recv_sem=fwd_recv.at[s],
            device_id={"rep": other},
            device_id_type=MESH,
        )

    order = list(range(1, sp))
    for k in order:
        feat_copy(k).start()
    fwd_copy(me, normed.at[me]).start()
    feats[me, rep] = normed[me]

    token_base = blk * span
    lanes = lax.broadcasted_iota(jnp.int32, (1, HEAD), 1)
    index = lax.rem(lanes, HEAD // 2).astype(F32)
    inverse = jnp.exp(index * (-2.0 * math.log(THETA_BASE) / HEAD))
    sign = jnp.where(lanes < HEAD // 2, -1.0, 1.0)

    def angle_step(j, carry):
        at = pl.ds(pl.multiple_of(j * rows, rows), rows)
        places = token_base + j * rows + lax.broadcasted_iota(jnp.int32, (rows, HEAD), 0)
        angles = places.astype(F32) * inverse
        cos_buf[at, :] = jnp.cos(angles)
        sin_buf[at, :] = jnp.sin(angles) * sign
        return carry

    lax.fori_loop(0, sp, angle_step, 0)
    load_k.wait()
    load_v.wait()

    def rows_of(j):
        return pl.ds(pl.multiple_of(j * rows, rows), rows)

    def pair_copy(slot, j):
        return pltpu.make_async_remote_copy(
            src_ref=part_out.at[slot_head(slot, 1 - parity), rows_of(j)],
            dst_ref=pair_in.at[slot, rows_of(j)],
            send_sem=pair_send.at[slot],
            recv_sem=pair_recv.at[slot, j],
            device_id={"sp": partner},
            device_id_type=MESH,
        )

    def part_copy(d, j):
        slot = d // fold if fold > 1 else d // 2
        return pltpu.make_async_remote_copy(
            src_ref=pair_out.at[slot, rows_of(j)],
            dst_ref=part_in.at[my_pair, rows_of(j)],
            send_sem=part_send.at[d // 2],
            recv_sem=part_recv.at[my_pair, j],
            device_id={"sp": d},
            device_id_type=MESH,
        )

    def far(k):
        return 2 * lax.rem(my_pair + k, pairs) + parity

    def project(j):
        at = rows_of(j)
        block = feats[j].reshape(rows, fs)
        partial = jnp.dot(block, wts[...], preferred_element_type=F32)
        for h in range(kv_heads):
            key_part = partial[:, h * HEAD : (h + 1) * HEAD]
            value_part = partial[:, (kv_heads + h) * HEAD : (kv_heads + h + 1) * HEAD]
            part_own[h, at, :HEAD] = key_part
            part_own[h, at, HEAD:] = value_part
            part_out[h, at, :HEAD] = key_part.astype(BF16)
            part_out[h, at, HEAD:] = value_part.astype(BF16)
        for slot in range(slots):
            pair_copy(slot, j).start()

    def cross(j):
        at = rows_of(j)
        for slot in range(slots):
            pair_copy(slot, j).wait_recv()
            both = part_own[slot_head(slot, parity), at, :] + pair_in[slot, at, :].astype(F32)
            part_own[slot_head(slot, parity), at, :] = both
            pair_out[slot, at, :] = both.astype(BF16)
        for k in range(1, pairs):
            part_copy(far(k), j).start()

    fwd_arrival(me).wait_recv()
    project(me)

    def arrive(k, carry):
        s = place(k)
        feat_arrival(s).wait_recv()
        fwd_copy(s, feats.at[s, rep]).start()
        fwd_arrival(s).wait_recv()
        project(s)
        cross(place(k - 1))
        return carry

    lax.fori_loop(1, sp, arrive, 0)
    cross(place(sp - 1))

    def q_copy(d):
        return pltpu.make_async_remote_copy(
            src_ref=queries_ref.at[0, :, pl.ds(pl.multiple_of(d * q_cols, q_cols), q_cols)],
            dst_ref=qbuf.at[me],
            send_sem=q_send.at[d],
            recv_sem=q_recv.at[me],
            device_id={"sp": d},
            device_id_type=MESH,
        )

    def q_arrival(s):
        return pltpu.make_async_remote_copy(
            src_ref=qbuf.at[s],
            dst_ref=qbuf.at[s],
            send_sem=q_send.at[s],
            recv_sem=q_recv.at[s],
            device_id={"sp": s},
            device_id_type=MESH,
        )

    for k in reversed(order):
        q_copy(peer(k)).start()

    for piece in (0, 1):

        @pl.when(blk < 2 - piece)
        def _():
            kv[pl.ds(piece * span, span), :] = jnp.zeros((span, 2 * HEAD), BF16)


    def own_shift(ref):
        row = ref[...].astype(F32).reshape(1, kv_heads * HEAD)
        mine = row[:, :HEAD]
        for h in range(1, kv_heads):
            mine = jnp.where(my_head == h, row[:, h * HEAD : (h + 1) * HEAD], mine)
        return mine

    key_shift = own_shift(kb_ref)
    value_shift = own_shift(vb_ref)

    relay = blks == 4

    def kv_copy(piece, dist, j):
        return pltpu.make_async_remote_copy(
            src_ref=kv.at[pl.ds(pl.multiple_of(piece * span + j * rows, rows), rows)],
            dst_ref=kv.at[pl.ds(pl.multiple_of((2 - dist) * span + j * rows, rows), rows)],
            send_sem=kv_send.at[dist - 1],
            recv_sem=kv_recv.at[dist - 1, j],
            device_id={"blk": lax.rem(blk + dist, blks)},
            device_id_type=MESH,
        )

    def kv_pass(j):
        kv_copy(2, 2, j).wait_recv()
        pltpu.make_async_remote_copy(
            src_ref=kv.at[pl.ds(pl.multiple_of(j * rows, rows), rows)],
            dst_ref=kv.at[pl.ds(pl.multiple_of(span + j * rows, rows), rows)],
            send_sem=kv_send.at[0],
            recv_sem=kv_recv.at[0, j],
            device_id={"blk": lax.rem(blk + blks - 1, blks)},
            device_id_type=MESH,
        ).start()

    near = blk + 1 < blks
    if relay:
        near = near & (blk != 1)
    sends = {1: near, 2: blk + 2 < blks}

    def finish(i, carry):
        j = place(i)
        at = rows_of(j)
        total = part_own[my_head, at, :]
        for k in range(1, pairs):
            s = lax.rem(my_pair + k, pairs)
            pltpu.make_async_remote_copy(
                src_ref=part_in.at[s, at],
                dst_ref=part_in.at[s, at],
                send_sem=part_send.at[s],
                recv_sem=part_recv.at[s, j],
                device_id={"sp": far(k)},
                device_id_type=MESH,
            ).wait_recv()
            total = total + part_in[s, at, :].astype(F32)
        keys = total[:, :HEAD] + key_shift
        turned = keys * cos_buf[at, :] + pltpu.roll(keys, HEAD // 2, 1) * sin_buf[at, :]
        put = pl.ds(pl.multiple_of(2 * span + j * rows, rows), rows)
        kv[put, :HEAD] = turned.astype(BF16)
        kv[put, HEAD:] = (total[:, HEAD:] + value_shift).astype(BF16)
        for dist in (2, 1):

            @pl.when(sends[dist])
            def _():
                kv_copy(2, dist, j).start()

        if relay:

            @pl.when((blk == 3) & (i >= 1))
            def _():
                kv_pass(place(i - 1))

        return carry

    lax.fori_loop(0, sp, finish, 0)
    if relay:

        @pl.when(blk == 3)
        def _():
            kv_pass(place(sp - 1))


    ends = []
    running = jnp.int32(0)
    for d in range(docs):
        running = running + docs_ref[d]
        ends.append(running)

    load_q.wait()
    for dist in (1, 2):

        arrives = blk >= dist
        if relay and dist == 2:
            arrives = arrives & (blk != 3)

        @pl.when(arrives)
        def _():
            for j in range(sp):
                kv_copy(2, dist, j).wait_recv()

    exponent = math.log2(math.e) / math.sqrt(HEAD)

    def attend(t):
        query_at = token_base + t * rows + lax.broadcasted_iota(jnp.int32, (rows, HEAD), 0)
        first = jnp.zeros((rows, HEAD), jnp.int32)
        for end in ends:
            first = jnp.where(query_at >= end, end, first)
        key_base = token_base - 2 * span + t * rows
        for c in range(window // HEAD):
            key_at = key_base + c * HEAD + lax.broadcasted_iota(jnp.int32, (rows, HEAD), 1)
            seen = (key_at >= first) & (key_at <= query_at)
            mask_buf[:, c * HEAD : (c + 1) * HEAD] = jnp.where(seen, 0.0, NEG_FILL)
        at = pl.ds(pl.multiple_of(t * rows, rows), window)
        for h in range(heads):
            cols = slice(h * HEAD, (h + 1) * HEAD)
            scores = lax.dot_general(
                qbuf[t, :, cols], kv[at, :HEAD], (((1,), (1,)), ((), ())), preferred_element_type=F32
            )
            scores = scores + mask_buf[...]
            largest = jnp.max(scores, axis=1, keepdims=True)
            weights = jnp.exp2((scores - largest) * exponent).astype(BF16)
            total = jnp.sum(weights.astype(F32), axis=1, keepdims=True)
            summed = jnp.dot(weights, kv[at, HEAD:], preferred_element_type=F32)
            obuf[t, :, cols] = (summed / total).astype(BF16)

    my_cols = pl.ds(pl.multiple_of(me * q_cols, q_cols), q_cols)

    def o_copy(d):
        return pltpu.make_async_remote_copy(
            src_ref=obuf.at[d],
            dst_ref=out_ref.at[0, :, my_cols],
            send_sem=o_send.at[d],
            recv_sem=o_recv.at[me],
            device_id={"sp": d},
            device_id_type=MESH,
        )

    def o_arrival(s):
        return pltpu.make_async_remote_copy(
            src_ref=obuf.at[s],
            dst_ref=out_ref.at[0, :, pl.ds(pl.multiple_of(s * q_cols, q_cols), q_cols)],
            send_sem=o_send.at[s],
            recv_sem=o_recv.at[s],
            device_id={"sp": s},
            device_id_type=MESH,
        )

    def each(k, carry):
        t = place(sp - k)
        q_arrival(t).wait_recv()
        attend(t)
        o_copy(t).start()
        return carry

    lax.fori_loop(1, sp, each, 0)
    attend(me)
    out_ref[0, :, my_cols] = obuf[me]

    for k in order:
        d = peer(k)
        o_arrival(d).wait_recv()
        o_copy(d).wait_send()
        feat_copy(k).wait_send()
        q_copy(d).wait_send()
        fwd_copy(d, feats.at[d, rep]).wait_send()
    fwd_copy(me, normed.at[me]).wait_send()

    def sent(sem, source):
        pltpu.make_async_remote_copy(
            src_ref=source,
            dst_ref=source,
            send_sem=sem,
            recv_sem=part_recv.at[0, 0],
            device_id={"sp": partner},
            device_id_type=MESH,
        ).wait_send()

    for slot in range(slots):
        sent(pair_send.at[slot], pair_in.at[slot])
    for k in range(1, pairs):
        sent(part_send.at[far(k) // 2], part_in.at[0])
    for dist in (1, 2):

        shipped = sends[dist]
        if relay and dist == 1:
            shipped = shipped | (blk == 3)

        @pl.when(shipped)
        def _():
            sent(kv_send.at[dist - 1], kv.at[pl.ds(0, span)])


def heads_kernel(
    sizes,
    hidden_ref,
    queries_ref,
    gain_ref,
    kw_ref,
    vw_ref,
    kb_ref,
    vb_ref,
    docs_ref,
    out_ref,
    hid,
    wts,
    normed,
    feats,
    own,
    up_in,
    up_out,
    down_in,
    down_out,
    self_out,
    self_in,
    up_last,
    down_last,
    kv,
    qbuf,
    obuf,
    total,
    cos_buf,
    sin_buf,
    mask_buf,
    load_sem,
    feat_send,
    feat_recv,
    fwd_send,
    fwd_recv,
    q_send,
    q_recv,
    self_send,
    self_recv,
    up_send,
    up_recv,
    up_last_send,
    up_last_recv,
    down_send,
    down_recv,
    down_last_send,
    down_last_recv,
    rise_send,
    rise_recv,
    fall_send,
    fall_recv,
    o_send,
    o_recv,
):
    sp, blks, reps, rows, chunks = sizes
    me = lax.axis_index("sp")
    blk = lax.axis_index("blk")
    rep = lax.axis_index("rep")
    span = sp * rows
    cut = rows // chunks
    part = cut // reps
    fs = kw_ref.shape[0]
    q_cols = queries_ref.shape[2] // blks
    heads = q_cols // HEAD
    docs = docs_ref.shape[0]
    window = 2 * span + rows
    last = sp - 1
    pair = 2 * HEAD

    turn = 2 * lax.rem(blk, 2) - 1

    def group(k):
        return lax.rem(blk + blks + k * turn, blks)

    barrier = pltpu.get_barrier_semaphore()
    for k in range(1, sp):
        pl.semaphore_signal(
            barrier, inc=1, device_id={"sp": lax.rem(me + k, sp)}, device_id_type=MESH
        )
    for k in range(1, reps):
        pl.semaphore_signal(
            barrier, inc=1, device_id={"rep": lax.rem(rep + k, reps)}, device_id_type=MESH
        )
    for k in range(1, blks):
        pl.semaphore_signal(barrier, inc=1, device_id={"blk": group(k)}, device_id_type=MESH)

        @pl.when(me > 0)
        def _():
            pl.semaphore_signal(
                barrier, inc=1, device_id={"sp": me - 1, "blk": group(k)}, device_id_type=MESH
            )

        @pl.when(me < last)
        def _():
            pl.semaphore_signal(
                barrier, inc=1, device_id={"sp": me + 1, "blk": group(k)}, device_id_type=MESH
            )

    def load_hid(q):
        return pltpu.make_async_copy(
            hidden_ref.at[0, pl.ds(pl.multiple_of(q * cut + rep * part, part), part)],
            hid.at[q],
            load_sem.at[q],
        )

    def load_w(g, side):
        source = vw_ref if side else kw_ref
        return pltpu.make_async_copy(
            source.at[:, g * HEAD : (g + 1) * HEAD],
            wts.at[:, (2 * g + side) * HEAD : (2 * g + side + 1) * HEAD],
            load_sem.at[chunks + 2 * g + side],
        )

    own_cols = pl.ds(pl.multiple_of(blk * q_cols, q_cols), q_cols)
    load_q = pltpu.make_async_copy(
        queries_ref.at[0, :, own_cols], qbuf.at[blk], load_sem.at[chunks + 2 * blks]
    )
    for q in range(chunks):
        load_hid(q).start()
    for g in range(blks):
        load_w(g, 0).start()
        load_w(g, 1).start()
    load_q.start()

    def feat_copy(q, d):
        return pltpu.make_async_remote_copy(
            src_ref=normed.at[q, d],
            dst_ref=feats.at[q, me, rep],
            send_sem=feat_send,
            recv_sem=feat_recv.at[q, me],
            device_id={"sp": d},
            device_id_type=MESH,
        )

    def feat_arrival(q, s):
        return pltpu.make_async_remote_copy(
            src_ref=normed.at[q, 0],
            dst_ref=feats.at[q, s, rep],
            send_sem=feat_send,
            recv_sem=feat_recv.at[q, s],
            device_id={"sp": s},
            device_id_type=MESH,
        )

    other = lax.rem(rep + 1, reps)

    def fwd_copy(q, s, source):
        return pltpu.make_async_remote_copy(
            src_ref=source,
            dst_ref=feats.at[q, s, rep],
            send_sem=fwd_send,
            recv_sem=fwd_recv.at[q],
            device_id={"rep": other},
            device_id_type=MESH,
        )

    def q_copy(g):
        return pltpu.make_async_remote_copy(
            src_ref=queries_ref.at[0, :, pl.ds(pl.multiple_of(g * q_cols, q_cols), q_cols)],
            dst_ref=qbuf.at[blk],
            send_sem=q_send,
            recv_sem=q_recv,
            device_id={"blk": g},
            device_id_type=MESH,
        )

    def norm(q):
        load_hid(q).wait()
        values = hid[q].astype(F32)
        scale = lax.rsqrt(jnp.mean(values * values, axis=1, keepdims=True) + EPS_VALUE)
        for d in range(sp):
            cols = slice(d * fs, (d + 1) * fs)
            normed[q, d] = (hid[q, :, cols].astype(F32) * scale * gain_ref[:, cols]).astype(BF16)

    norm(0)
    peers = sp - 1 + reps - 1 + blks - 1

    @pl.when((me == 0) | (me == last))
    def _():
        pl.semaphore_wait(barrier, peers + blks - 1)

    @pl.when((me > 0) & (me < last))
    def _():
        pl.semaphore_wait(barrier, peers + 2 * (blks - 1))

    for q in range(chunks):
        if q > 0:
            norm(q)
        for step in range(1, sp):
            far = jnp.where(rep == 0, step, sp - step)

            @pl.when(me + far < sp)
            def _():
                feat_copy(q, me + far).start()

            @pl.when(me >= far)
            def _():
                feat_copy(q, me - far).start()

        fwd_copy(q, me, normed.at[q, me]).start()
        feats[q, me, rep] = normed[q, me]
    for k in range(1, blks):
        q_copy(group(k)).start()

    lanes = lax.broadcasted_iota(jnp.int32, (1, HEAD), 1)
    index = lax.rem(lanes, HEAD // 2).astype(F32)
    inverse = jnp.exp(index * (-2.0 * math.log(THETA_BASE) / HEAD))
    sign = jnp.where(lanes < HEAD // 2, -1.0, 1.0)

    def angle_step(c, carry):
        places = c * span + me * rows + lax.broadcasted_iota(jnp.int32, (rows, HEAD), 0)
        angles = places.astype(F32) * inverse
        cos_buf[c] = jnp.cos(angles)
        sin_buf[c] = jnp.sin(angles) * sign
        return carry

    lax.fori_loop(0, blks, angle_step, 0)
    kv[: 2 * span, :pair] = jnp.zeros((2 * span, pair), BF16)
    kv[:, pair:] = jnp.ones((kv.shape[0], HEAD), BF16)

    def own_shift(ref):
        row = ref[...].astype(F32).reshape(1, blks * HEAD)
        mine = row[:, :HEAD]
        for g in range(1, blks):
            mine = jnp.where(blk == g, row[:, g * HEAD : (g + 1) * HEAD], mine)
        return mine

    key_shift = own_shift(kb_ref)
    value_shift = own_shift(vb_ref)

    def landed(sem, ref):
        pltpu.make_async_remote_copy(
            src_ref=ref,
            dst_ref=ref,
            send_sem=sem,
            recv_sem=sem,
            device_id={"rep": other},
            device_id_type=MESH,
        ).wait_recv()

    def left(sem, ref):
        pltpu.make_async_remote_copy(
            src_ref=ref,
            dst_ref=ref,
            send_sem=sem,
            recv_sem=sem,
            device_id={"rep": other},
            device_id_type=MESH,
        ).wait_send()

    def self_copy(q, g):
        return pltpu.make_async_remote_copy(
            src_ref=self_out.at[q, g],
            dst_ref=self_in.at[q, blk],
            send_sem=self_send,
            recv_sem=self_recv.at[q],
            device_id={"blk": g},
            device_id_type=MESH,
        )

    def project(q):
        for far in range(1, sp):

            @pl.when(me >= far)
            def _():
                feat_arrival(q, me - far).wait_recv()
                fwd_copy(q, me - far, feats.at[q, me - far, rep]).start()

            @pl.when(me + far < sp)
            def _():
                feat_arrival(q, me + far).wait_recv()
                fwd_copy(q, me + far, feats.at[q, me + far, rep]).start()

        landed(fwd_recv.at[q], normed.at[q])
        partial = jnp.dot(
            feats[q].reshape(sp * cut, fs), wts[...], preferred_element_type=F32
        )
        for j in range(sp):
            for g in range(blks):
                own[q, j, g] = partial[j * cut : (j + 1) * cut, g * pair : (g + 1) * pair]

    def keep(q):
        for k in range(1, blks):
            g = group(k)
            self_out[q, g] = own[q, me, g].astype(BF16)
            self_copy(q, g).start()
        self_in[q, blk] = own[q, me, blk].astype(BF16)

    def hop(q, t, d, up):
        to = t + 1 if up else t - 1
        came = t > 0 if up else t < last
        inbound, outbound = (up_in, up_out) if up else (down_in, down_out)
        sent, arrived = (up_send, up_recv) if up else (down_send, down_recv)
        lands = up_last if up else down_last
        land_sent, landed_sem = (up_last_send, up_last_recv) if up else (down_last_send, down_last_recv)
        if came:
            landed(arrived.at[q, d], inbound.at[q, d])
        for g in range(blks):
            value = own[q, d, g]
            if came:
                value = value + inbound[q, d, g].astype(F32)
            outbound[q, d, g] = value.astype(BF16)
        if d != to:
            pltpu.make_async_remote_copy(
                src_ref=outbound.at[q, d],
                dst_ref=inbound.at[q, d],
                send_sem=sent,
                recv_sem=arrived.at[q, d],
                device_id={"sp": to},
                device_id_type=MESH,
            ).start()
        else:
            for k in range(blks):
                g = group(k)
                pltpu.make_async_remote_copy(
                    src_ref=outbound.at[q, d, g],
                    dst_ref=lands.at[q, blk],
                    send_sem=land_sent,
                    recv_sem=landed_sem.at[q],
                    device_id={"sp": to, "blk": g},
                    device_id_type=MESH,
                ).start()

    def relay(q, t, d):
        @pl.when(me == t)
        def _():
            hop(q, t, d, True)

        @pl.when(me == last - t)
        def _():
            hop(q, last - t, last - d, False)

    def place(q, c, j):
        return pl.ds(pl.multiple_of(2 * span + (c * sp + j) * rows + q * cut, cut), cut)

    sent_cols = slice(0, pair)

    def rise(q, j):
        for c in range(blks):
            pltpu.make_async_remote_copy(
                src_ref=kv.at[place(q, c, j), sent_cols],
                dst_ref=kv.at[place(q, c, j), sent_cols],
                send_sem=rise_send,
                recv_sem=rise_recv.at[q, j],
                device_id={"sp": me + 1},
                device_id_type=MESH,
            ).start()

    def fall(q, j):
        for c in range(blks - 1):
            pltpu.make_async_remote_copy(
                src_ref=kv.at[place(q, c, j), sent_cols],
                dst_ref=kv.at[place(q, c, j), sent_cols],
                send_sem=fall_send,
                recv_sem=fall_recv.at[q, j],
                device_id={"sp": me - 1},
                device_id_type=MESH,
            ).start()

    def close(q):
        landed(self_recv.at[q], self_in.at[q, pl.ds(0, blks - 1)])
        total[...] = self_in[q].astype(F32)

        @pl.when(me > 0)
        def _():
            landed(up_last_recv.at[q], up_last.at[q])
            total[...] = total[...] + up_last[q].astype(F32)

        @pl.when(me < last)
        def _():
            landed(down_last_recv.at[q], down_last.at[q])
            total[...] = total[...] + down_last[q].astype(F32)

        at = slice(q * cut, (q + 1) * cut)
        for c in range(blks):
            keys = total[c, :, :HEAD] + key_shift
            turned = keys * cos_buf[c, at] + pltpu.roll(keys, HEAD // 2, 1) * sin_buf[c, at]
            kv[place(q, c, me), :HEAD] = turned.astype(BF16)
            kv[place(q, c, me), HEAD:pair] = (total[c, :, HEAD:] + value_shift).astype(BF16)

        @pl.when(me < last)
        def _():
            rise(q, me)

        @pl.when(me > 0)
        def _():
            fall(q, me)

    def close_inner(q):
        @pl.when((me > 0) & (me < last))
        def _():
            close(q)

    def close_outer(q):
        @pl.when((me == 0) | (me == last))
        def _():
            close(q)

    every = kv.at[pl.ds(0, blks * cut), sent_cols]
    fallen = kv.at[pl.ds(0, (blks - 1) * cut), sent_cols]

    def gather(q, t, j):
        @pl.when(me == t)
        def _():
            landed(rise_recv.at[q, j], every)
            if t < last:
                rise(q, j)

        @pl.when(me == last - t)
        def _():
            landed(fall_recv.at[q, last - j], fallen)
            if t < last:
                fall(q, last - j)

    ends = []
    running = jnp.int32(0)
    for d in range(docs):
        running = running + docs_ref[d]
        ends.append(running)

    exponent = math.log2(math.e) / math.sqrt(HEAD)

    def mask_step(c, carry):
        query_at = c * span + me * rows + lax.broadcasted_iota(jnp.int32, (rows, HEAD), 0)
        first = jnp.zeros((rows, HEAD), jnp.int32)
        for end in ends:
            first = jnp.where(query_at >= end, end, first)
        base = c * span + me * rows - 2 * span
        for piece in range(window // HEAD):
            key_at = base + piece * HEAD + lax.broadcasted_iota(jnp.int32, (rows, HEAD), 1)
            seen = (key_at >= first) & (key_at <= query_at)
            mask_buf[c, :, piece * HEAD : (piece + 1) * HEAD] = jnp.where(seen, 0.0, NEG_FILL)
        return carry

    def attend(c):
        at = pl.ds(pl.multiple_of(c * span + me * rows, rows), window)
        for h in range(0, heads, 2):
            parts = [slice(n * HEAD, (n + 1) * HEAD) for n in range(h, min(h + 2, heads))]
            stacked = jnp.concatenate([qbuf[c, :, cols] for cols in parts], axis=0)
            scores = lax.dot_general(
                stacked, kv[at, :HEAD], (((1,), (1,)), ((), ())), preferred_element_type=F32
            )
            scores = scores.reshape(len(parts), rows, window) + mask_buf[c][None]
            scores = scores.reshape(len(parts) * rows, window)
            largest = jnp.max(scores, axis=1, keepdims=True)
            weights = jnp.exp2((scores - largest) * exponent).astype(BF16)
            summed = jnp.dot(weights, kv[at, HEAD:], preferred_element_type=F32)
            result = (summed[:, :HEAD] / summed[:, HEAD:]).astype(BF16)
            for n, cols in enumerate(parts):
                obuf[c, :, cols] = result[n * rows : (n + 1) * rows]

    def o_copy(c):
        return pltpu.make_async_remote_copy(
            src_ref=obuf.at[c],
            dst_ref=out_ref.at[0, :, own_cols],
            send_sem=o_send,
            recv_sem=o_recv,
            device_id={"blk": c},
            device_id_type=MESH,
        )

    def weights_in():
        for g in range(blks):
            load_w(g, 0).wait()
            load_w(g, 1).wait()

    def queries_in():
        load_q.wait()
        landed(q_recv, qbuf.at[pl.ds(0, blks - 1)])

    def finish(k, carry):
        attend(group(k))
        o_copy(group(k)).start()
        return carry

    unit, hop_time, lead = 5.6 / chunks, 3.3, 13.0
    inner_late, outer_late, gather_late, first_late = 1.0, 0.0, 4.0, 0.0
    hold = 0
    feed_first, feed_step = 10.0, 11.2 / chunks
    queue = []
    for q in range(chunks + hold):
        if q < chunks:
            queue.append((q, last))
        if q >= hold and hold:
            queue.append((q - hold, 1))
        if q < chunks:
            queue.extend((q, d) for d in range(last - 1, 0 if not hold else 1, -1))
    came = {item: lead + unit * (n + 1) + 1.0 for n, item in enumerate(queue)}
    fed = lead + unit * len(queue) + 1.0
    events = []
    for q in range(chunks):

        def first_step(q=q):
            if q == 0:
                weights_in()
            project(q)
            begin = queue.index((q, last))
            end = queue.index((q + 1, last)) if q + 1 < chunks else len(queue)
            for n in range(begin, end):
                relay(queue[n][0], 0, queue[n][1])
            keep(q)

        events.append((feed_first + feed_step * q, first_step, ()))
        for t in range(1, last):
            for d in range(last, t, -1):
                events.append((came[q, d] + hop_time * (t - 1), relay, (q, t, d)))
        inner = max(came[q, 1], came[q, last - 1] + hop_time) + inner_late
        outer = came[q, last] + hop_time * (last - 1) + outer_late
        events.append((inner, close_inner, (q,)))
        events.append((outer, close_outer, (q,)))
        for j in range(last):
            for t in range(j + 1, sp):
                if j == 0:
                    come = max(outer + hop_time, fed + unit * (q + 1)) + first_late
                else:
                    come = inner + hop_time + gather_late
                when = come + (t - j - 1) * hop_time
                events.append((1000.0 + when if t == last else when, gather, (q, t, j)))

    def masks_outer():
        @pl.when((me == 0) | (me == last))
        def _():
            lax.fori_loop(0, blks, mask_step, 0)

    def masks_inner():
        @pl.when((me > 0) & (me < last))
        def _():
            lax.fori_loop(0, blks, mask_step, 0)

    events.append((feed_first + feed_step * (chunks - 1) + 0.1, masks_outer, ()))
    events.append((999.0, masks_inner, ()))
    events.sort(key=lambda e: e[0])
    for _, step, taken in events:
        step(*taken)
    queries_in()

    lax.fori_loop(1, blks, finish, 0)
    attend(blk)
    out_ref[0, :, own_cols] = obuf[blk]

    some = pl.ds(0, blks - 1)
    left(feat_send, normed.at[:, pl.ds(0, sp - 1)])
    left(fwd_send, normed)
    left(self_send, self_out.at[:, some])
    left(q_send, qbuf.at[some])
    for t in range(sp):

        @pl.when(me == t)
        def _():
            if t < last - 1:
                left(up_send, up_out.at[:, pl.ds(0, last - t - 1)])
            if t > 1:
                left(down_send, down_out.at[:, pl.ds(0, t - 1)])
            if t < last:
                left(up_last_send, up_last)
                left(rise_send, kv.at[pl.ds(0, blks * rows * (t + 1)), sent_cols])
            if t > 0:
                left(down_last_send, down_last)
                left(fall_send, kv.at[pl.ds(0, (blks - 1) * rows * (sp - t)), sent_cols])

    landed(o_recv, obuf.at[some])
    left(o_send, obuf.at[some])


CHUNKS = 4


def heads_call(operands, sp, blks, reps):
    hidden, queries, _, key_matrix = operands[:4]
    rows, width = hidden.shape[1:]
    chunks = CHUNKS
    cut = rows // chunks
    span = rows * sp
    fs, kv_cols = key_matrix.shape
    q_cols = queries.shape[2] // blks
    pair = 2 * HEAD
    vmem = pl.BlockSpec(memory_space=pltpu.VMEM)
    anywhere = pl.BlockSpec(memory_space=pl.ANY)
    smem = pl.BlockSpec(memory_space=pltpu.SMEM)
    dma = pltpu.SemaphoreType.DMA
    by_sp, each = dma((chunks, sp)), dma((chunks,))
    line = pltpu.VMEM((chunks, sp, blks, cut, pair), BF16)
    spot = pltpu.VMEM((chunks, blks, cut, pair), BF16)
    return pl.pallas_call(
        functools.partial(heads_kernel, (sp, blks, reps, rows, chunks)),
        out_shape=pltpu.VMEM(queries.shape, BF16),
        in_specs=[anywhere, anywhere, vmem, anywhere, anywhere, vmem, vmem, smem],
        out_specs=vmem,
        scratch_shapes=[
            pltpu.VMEM((chunks, cut // reps, width), BF16),
            pltpu.VMEM((fs, 2 * kv_cols), BF16),
            pltpu.VMEM((chunks, sp, cut // reps, fs), BF16),
            pltpu.VMEM((chunks, sp, reps, cut // reps, fs), BF16),
            pltpu.VMEM((chunks, sp, blks, cut, pair), F32),
            line,
            line,
            line,
            line,
            spot,
            spot,
            spot,
            spot,
            pltpu.VMEM(((2 + blks) * span, 3 * HEAD), BF16),
            pltpu.VMEM((blks, rows, q_cols), BF16),
            pltpu.VMEM((blks, rows, q_cols), BF16),
            pltpu.VMEM((blks, cut, pair), F32),
            pltpu.VMEM((blks, rows, HEAD), F32),
            pltpu.VMEM((blks, rows, HEAD), F32),
            pltpu.VMEM((blks, rows, 2 * span + rows), F32),
            dma((chunks + 2 * blks + 1,)),
            dma,
            by_sp,
            dma,
            each,
            dma,
            dma,
            dma,
            each,
            dma,
            by_sp,
            dma,
            each,
            dma,
            by_sp,
            dma,
            each,
            dma,
            by_sp,
            dma,
            by_sp,
            dma,
            dma,
        ],
        compiler_params=pltpu.CompilerParams(
            collective_id=0, has_side_effects=True, vmem_limit_bytes=60 * 1024 * 1024
        ),
        name="masked_attention",
    )(*operands)


def on_device(
    hidden,
    queries,
    norm_gain,
    key_matrix,
    value_matrix,
    key_shift_bias,
    value_shift_bias,
    doc_lengths,
):
    sp = lax.axis_size("sp")
    blks = lax.axis_size("blk")
    reps = lax.axis_size("rep")
    rows, width = hidden.shape[1:]
    half = rows // reps
    span = rows * sp
    fs = key_matrix.shape[0]
    kv_cols = key_matrix.shape[1]
    kv_heads = kv_cols // HEAD
    q_cols = queries.shape[2] // sp
    window = 2 * span + rows
    slots = kv_heads if sp > kv_heads else kv_heads // 2
    operands = (
        hidden,
        queries,
        norm_gain.reshape(1, width),
        key_matrix,
        value_matrix,
        key_shift_bias,
        value_shift_bias,
        doc_lengths,
    )
    if blks == kv_heads:
        return heads_call(operands, sp, blks, reps)
    vmem = pl.BlockSpec(memory_space=pltpu.VMEM)
    anywhere = pl.BlockSpec(memory_space=pl.ANY)
    smem = pl.BlockSpec(memory_space=pltpu.SMEM)
    dma = pltpu.SemaphoreType.DMA
    return pl.pallas_call(
        functools.partial(kernel, (sp, blks, reps, rows)),
        out_shape=jax.ShapeDtypeStruct(queries.shape, BF16),
        in_specs=[anywhere, anywhere, vmem, anywhere, anywhere, vmem, vmem, smem],
        out_specs=vmem,
        scratch_shapes=[
            pltpu.VMEM((half, width), BF16),
            pltpu.VMEM((fs, 2 * kv_cols), BF16),
            pltpu.VMEM((sp, half, fs), BF16),
            pltpu.VMEM((sp, reps, half, fs), BF16),
            pltpu.VMEM((kv_heads, span, 2 * HEAD), F32),
            pltpu.VMEM((kv_heads, span, 2 * HEAD), BF16),
            pltpu.VMEM((slots, span, 2 * HEAD), BF16),
            pltpu.VMEM((slots, span, 2 * HEAD), BF16),
            pltpu.VMEM((sp // 2, span, 2 * HEAD), BF16),
            pltpu.VMEM((3 * span, 2 * HEAD), BF16),
            pltpu.VMEM((sp, rows, q_cols), BF16),
            pltpu.VMEM((sp, rows, q_cols), BF16),
            pltpu.VMEM((span, HEAD), F32),
            pltpu.VMEM((span, HEAD), F32),
            pltpu.VMEM((rows, window), F32),
            dma((4,)),
            dma((sp,)),
            dma((sp,)),
            dma((sp,)),
            dma((sp,)),
            dma((sp,)),
            dma((sp,)),
            dma((slots,)),
            dma((slots, sp)),
            dma((sp // 2,)),
            dma((sp // 2, sp)),
            dma((2,)),
            dma((2, sp)),
            dma((sp,)),
            dma((sp,)),
        ],
        compiler_params=pltpu.CompilerParams(
            collective_id=0, has_side_effects=True, vmem_limit_bytes=60 * 1024 * 1024
        ),
        name="masked_attention",
    )(*operands)


def solution(mesh):
    in_specs = (
        P(("grp", "blk"), "sp", None),
        P(("grp", "blk"), "sp", "rep"),
        P(),
        P("sp", "rep"),
        P("sp", "rep"),
        P("rep"),
        P("rep"),
        P("grp"),
    )
    out_specs = P(("grp", "blk"), "sp", "rep")
    return jax.shard_map(
        on_device, mesh=mesh, in_specs=in_specs, out_specs=out_specs, check_vma=False
    )
```
